128 devices in a mesh: dp: 8 (over x, core), mp: 16 (over z, y).
Axes of the slice: x: 4, y: 4, z: 4, core: 2. Of those that a mesh axis runs over, the one named last changes fastest.
Arguments:
- tokens: bfloat16 [2048, 8192], P('dp'), may hold values from -6 to 6
- norm_gain: float32 [8192], replicated, may hold values from 0.5 to 1.5
- gate_weight: bfloat16 [8192, 28672], P('dp', 'mp'), may hold values from -0.0625 to 0.0625
- gate_mask: int32 [8192, 896], P('dp', 'mp'), may hold values from -2147483648 to 2147483646
- up_weight: bfloat16 [8192, 28672], P('dp', 'mp'), may hold values from -0.0625 to 0.0625
- up_mask: int32 [8192, 896], P('dp', 'mp'), may hold values from -2147483648 to 2147483646
- down_weight: bfloat16 [28672, 8192], P('mp', 'dp'), may hold values from -0.03125 to 0.03125
- down_mask: int32 [28672, 256], P('mp', 'dp'), may hold values from -2147483648 to 2147483647, as said below
Outputs:
- mixed: bfloat16 [2048, 8192], P('mp', 'dp')
- input_norms: float32 [8192], P('dp')
- hidden_norms: float32 [28672], P('mp')
The draws below stay inside these ranges and needn't reach their ends.
Inputs may be any that keep to these rules, and one draw needn't show every extreme that they name: `down_mask`: in every word each of the eight aligned groups of four bits holds exactly two ones, so exactly two of every four consecutive columns of the down projection are kept.
All inputs are finite; a program needn't handle non-finite values.
Results may differ from the reference program's by a relative error of at most 0.025.
Values may be sent and summed in bfloat16 or wider, within the bound.
A program may use at most 128 MiB of HBM per device.

```python
import jax
import jax.numpy as jnp
from jax import lax

D = 8192
FF = 28672
TOKENS = 2048
N_DP = 8
N_MP = 16


def draw_down_mask(key, part):
    patterns = jnp.array([3, 5, 6, 9, 10, 12], jnp.int32)
    selected = jax.random.randint(key, (FF, D // 32, 8), 0, 6, dtype=jnp.int32)
    nibbles = patterns[selected]
    shifts = 4 * jnp.arange(8, dtype=jnp.int32)
    placed = jnp.left_shift(nibbles, shifts)
    return jnp.sum(placed, axis=2, dtype=jnp.int32)


def set_ends(entries, rng, least, largest):
    longest = entries.shape.index(max(entries.shape))
    spots = []
    for shift in (0, 1):
        where = [jax.random.randint(jax.random.fold_in(rng, axis), (), 0, length) for axis, length in enumerate(entries.shape)]
        where[longest] = (where[longest] + shift) % entries.shape[longest]
        spots.append(tuple(where))
    return entries.at[spots[0]].set(least).at[spots[1]].set(largest)


def level_of(key, shape, split, smallest, high):
    def one(axis_at, blocks):
        heights = jax.random.uniform(jax.random.fold_in(jax.random.fold_in(key, 6), axis_at), (blocks,), jnp.float32, smallest / len(split), high / len(split))
        return jnp.repeat(jnp.exp(heights), shape[axis_at] // blocks).reshape((-1,) + (1,) * (len(shape) - axis_at - 1))

    level = one(*split[0])
    for cut in split[1:]:
        level = level * one(*cut)
    return level


def centred(stream_key, extent, width, most, cuts=(), kind=jnp.bfloat16):
    gain = level_of(stream_key, extent, cuts, -0.22, 0.18) if cuts else 1.0
    entries = jax.random.normal(stream_key, extent, jnp.float32) * width * gain
    return jnp.minimum(jnp.maximum(entries, -most), most).astype(kind)


def setup_inputs(seed: int = 0) -> dict:
    keys = jax.random.split(jax.random.key(seed), 9)
    tokens = centred(keys[0], (TOKENS, D), 1.0, 6.0, ((0, 8),))
    norm_gain = jnp.clip(1.0 + 0.1 * jax.random.normal(keys[1], (D,), jnp.float32), 0.5, 1.5)
    gate_weight = centred(keys[2], (D, FF), D ** -0.5, 0.0625, ((0, 8), (1, 16)))
    gate_mask = set_ends(jax.random.randint(keys[3], (D, FF // 32), -2147483648, 2147483647), jax.random.fold_in(keys[3], 1), -2147483648, 2147483646).astype(jnp.int32)
    up_weight = centred(keys[4], (D, FF), D ** -0.5, 0.0625, ((0, 8), (1, 16)))
    up_mask = set_ends(jax.random.randint(keys[5], (D, FF // 32), -2147483648, 2147483647), jax.random.fold_in(keys[5], 1), -2147483648, 2147483646).astype(jnp.int32)
    down_weight = centred(keys[6], (FF, D), FF ** -0.5, 0.03125, ((0, 16), (1, 8)))
    down_mask = draw_down_mask(jax.random.fold_in(keys[8], 71), 0)
    return dict(tokens=tokens, norm_gain=norm_gain, gate_weight=gate_weight, gate_mask=gate_mask, up_weight=up_weight, up_mask=up_mask, down_weight=down_weight, down_mask=down_mask)


def keep_entries(weight, packed):
    shifts = jnp.arange(32, dtype=jnp.int32)
    kept_bits = jnp.right_shift(packed[..., None], shifts) & 1
    kept_bits = kept_bits.reshape(weight.shape)
    return jnp.where(kept_bits == 1, weight, jnp.zeros_like(weight))

def reference(tokens, norm_gain, gate_weight, gate_mask, up_weight, up_mask, down_weight, down_mask):
    values = tokens.astype(jnp.float32)
    scale = lax.rsqrt(lax.optimization_barrier(jnp.mean(values * values, axis=1, keepdims=True)) + 1e-05)
    normed = (values * scale * norm_gain).astype(jnp.bfloat16)
    widened = normed.astype(jnp.float32)
    input_norms = jnp.sqrt(lax.optimization_barrier(jnp.sum(widened * widened, axis=0)))
    stride = D // N_DP

    def add_block(position, sums_so_far):
        gate_sum, up_sum = sums_so_far
        offset = (position * stride).astype(jnp.int32)
        row_block = lax.dynamic_slice_in_dim(normed, offset, stride, 1)
        gate_rows = keep_entries(lax.dynamic_slice_in_dim(gate_weight, offset, stride, 0), lax.dynamic_slice_in_dim(gate_mask, offset, stride, 0))
        up_rows = keep_entries(lax.dynamic_slice_in_dim(up_weight, offset, stride, 0), lax.dynamic_slice_in_dim(up_mask, offset, stride, 0))
        gate_part = jnp.dot(row_block, gate_rows, preferred_element_type=jnp.float32).astype(jnp.bfloat16)
        up_part = jnp.dot(row_block, up_rows, preferred_element_type=jnp.float32).astype(jnp.bfloat16)
        gate_part, up_part = lax.optimization_barrier((gate_part, up_part))
        return (gate_sum + gate_part.astype(jnp.float32), up_sum + up_part.astype(jnp.float32))
    zeros_sum = jnp.zeros((normed.shape[0], FF), jnp.float32)
    gate, up = lax.fori_loop(0, N_DP, add_block, (zeros_sum, zeros_sum))
    hidden = (jax.nn.silu(gate) * up).astype(jnp.bfloat16)
    wide_hidden = hidden.astype(jnp.float32)
    hidden_norms = jnp.sqrt(lax.optimization_barrier(jnp.sum(wide_hidden * wide_hidden, axis=0)))
    unit_stride = FF // N_MP

    def add_down(position, running):
        offset = (position * unit_stride).astype(jnp.int32)
        row_block = lax.dynamic_slice_in_dim(hidden, offset, unit_stride, 1)
        down_rows = keep_entries(lax.dynamic_slice_in_dim(down_weight, offset, unit_stride, 0), lax.dynamic_slice_in_dim(down_mask, offset, unit_stride, 0))
        return running + jnp.dot(row_block, down_rows, preferred_element_type=jnp.float32)
    mixed = lax.fori_loop(0, N_MP, add_down, jnp.zeros((normed.shape[0], D), jnp.float32))
    return (mixed.astype(jnp.bfloat16), input_norms, hidden_norms)
```

```python
import functools

import jax
import jax.numpy as jnp
from jax import lax
from jax.experimental import pallas as pl
from jax.experimental.pallas import tpu as pltpu
from jax.sharding import PartitionSpec as P

MESH = pl.DeviceIdType.MESH
BF = jnp.bfloat16
F32 = jnp.float32

NX = 4
G = 4
RT = 256
R = RT // G
H = R // 2
NT = 7
FC = 2048
UH = 896


def norm_kernel(tok_ref, gain_ref, out_ref):
    v = tok_ref[...].astype(F32)
    scale = lax.rsqrt(jnp.sum(v * v, axis=1, keepdims=True) * (1.0 / 8192) + 1e-05)
    n = (v * scale * gain_ref[...]).astype(BF)
    for i in range(NX):
        out_ref[i] = n[:, i * FC : (i + 1) * FC]


def norm_call(tokens, gain):
    return pl.pallas_call(
        norm_kernel,
        grid=(2 * G,),
        in_specs=[
            pl.BlockSpec((H, 8192), lambda b: (b, 0)),
            pl.BlockSpec((1, 8192), lambda b: (0, 0)),
        ],
        out_specs=pl.BlockSpec((NX, H, FC), lambda b: (0, (b % G) * 2 + b // G, 0)),
        out_shape=jax.ShapeDtypeStruct((NX, RT, FC), BF),
    )(tokens, gain.reshape(1, 8192))


def kept(words, weight, tile):
    lane = lax.broadcasted_iota(jnp.int32, words.shape, 1)
    spread = jnp.take_along_axis(
        words, 4 * tile + lane // 32, axis=1, mode="promise_in_bounds"
    )
    bit = lax.shift_right_logical(spread, lane % 32) & 1
    return jnp.where(bit == 1, weight.astype(F32), 0.0).astype(BF)


def mask_gu_kernel(gate, gmask, up, umask, out, gw, uw):
    gw[:, 0:56] = gmask[...]
    uw[:, 0:56] = umask[...]

    def body(r, carry):
        rows = pl.ds(pl.multiple_of(r * 32, 32), 32)
        g, u = gw[rows, :], uw[rows, :]
        for j in range(14):
            cols = slice(j * 128, (j + 1) * 128)
            out[j, rows, 0:128] = kept(g, gate[rows, cols], j)
            out[j, rows, 128:256] = kept(u, up[rows, cols], j)
        return carry

    lax.fori_loop(0, gate.shape[0] // 32, body, 0)


def mask_gu(gate, gmask, up, umask):
    rows = 256
    wide = pl.BlockSpec((rows, 1792), lambda b: (b, 0))
    thin = pl.BlockSpec((rows, 56), lambda b: (b, 0))
    return pl.pallas_call(
        mask_gu_kernel,
        grid=(1024 // rows,),
        in_specs=[wide, thin, wide, thin],
        out_specs=pl.BlockSpec((14, rows, 256), lambda b: (0, b, 0)),
        out_shape=jax.ShapeDtypeStruct((14, 1024, 256), BF),
        scratch_shapes=[pltpu.VMEM((rows, 128), jnp.int32)] * 2,
    )(gate, gmask, up, umask)


def mask_down_kernel(weight, mask, out, words):
    words[:, 0:32] = mask[...]

    def body(r, carry):
        rows = pl.ds(pl.multiple_of(r * 32, 32), 32)
        w = words[rows, :]
        for j in range(8):
            cols = slice(j * 128, (j + 1) * 128)
            out[rows, cols] = kept(w, weight[rows, cols], j)
        return carry

    lax.fori_loop(0, weight.shape[0] // 32, body, 0)


def mask_down(weight, mask):
    rows = 256
    return pl.pallas_call(
        mask_down_kernel,
        grid=(1792 // rows,),
        in_specs=[
            pl.BlockSpec((rows, 1024), lambda b: (b, 0)),
            pl.BlockSpec((rows, 32), lambda b: (b, 0)),
        ],
        out_specs=pl.BlockSpec((rows, 1024), lambda b: (b, 0)),
        out_shape=jax.ShapeDtypeStruct((1792, 1024), BF),
        scratch_shapes=[pltpu.VMEM((rows, 128), jnp.int32)],
    )(weight, mask)


def main_kernel(
    nrm, gu_h, dn_h,
    out, inorm, hnorm,
    gu, dn, tok, rs, hid, p, psend, drecv, isq, isq_r, hsq, hsq_r,
    w_loc, w_send, w_recv, dn_loc, dn_send, dn_recv, a_loc,
    ax_send, ax_recv, af_send, af_recv, rs_send, rs_recv, ag_send, ag_recv,
    d_send, d_recv, n_send, n_recv,
):
    dp, mp = lax.axis_index("dp"), lax.axis_index("mp")
    x, c = dp // 2, dp % 2
    z, y = mp // 4, mp % 4
    sends = []

    def xs(k):
        return lax.rem(x + k + 4, 4)

    def at(xx, cc, zz, yy):
        return (xx * 2 + cc, zz * 4 + yy)

    peer = at(x, 1 - c, z, y)

    def remote(src, dst, ssem, rsem, dev):
        return pltpu.make_async_remote_copy(
            src_ref=src, dst_ref=dst, send_sem=ssem, recv_sem=rsem,
            device_id=dev, device_id_type=MESH,
        )

    def go(copy):
        copy.start()
        sends.append(copy)
        return copy

    mine = pl.ds(pl.multiple_of(c * 1024, 1024), 1024)

    def w_local(t):
        return pltpu.make_async_copy(gu_h.at[t], gu.at[t, mine], w_loc.at[t])

    def w_remote(t):
        return remote(gu_h.at[t], gu.at[t, mine], w_send.at[t], w_recv.at[t], peer)

    own = pltpu.make_async_copy(nrm.at[x], tok.at[x], a_loc.at[0])
    own.start()

    def load(n, carry):
        w_local(n).start()
        w_local(NT + n).start()
        return carry

    lax.fori_loop(0, NT, load, 0)
    dn_local = pltpu.make_async_copy(dn_h, dn.at[c], dn_loc.at[0])
    dn_local.start()

    barrier = pltpu.get_barrier_semaphore()
    for k in (1, 2, 3):
        pl.semaphore_signal(barrier, inc=1, device_id=at(xs(k), c, z, y), device_id_type=MESH)

    def greet(k, carry):
        other = lax.rem(c * 16 + mp + k, 32)
        pl.semaphore_signal(
            barrier, inc=1, device_id=(x * 2 + other // 16, other % 16), device_id_type=MESH
        )
        return carry

    lax.fori_loop(1, 32, greet, 0)
    pl.semaphore_wait(barrier, 34)

    def coord(g):
        return y if g % 2 == 0 else z

    def piece(g, w):
        return pl.ds(pl.multiple_of(g * R + w * 16, 16), 16)

    def ax(g, dx):
        rows = piece(g, coord(g))
        return remote(
            nrm.at[xs(dx), rows], tok.at[x, rows],
            ax_send.at[g, dx - 1], ax_recv.at[g, dx - 1], at(xs(dx), c, z, y),
        )

    def af(g, dx, dw):
        src = xs(-dx)
        rows = piece(g, coord(g))
        w = lax.rem(coord(g) + dw, 4)
        dev = at(x, c, z, w) if g % 2 == 0 else at(x, c, w, y)
        return remote(
            tok.at[src, rows], tok.at[src, rows],
            af_send.at[g, dx - 1, dw - 1], af_recv.at[g, dx - 1, dw - 1], dev,
        )

    for dx in (1, 3, 2):
        go(ax(0, dx))

    def send_w(n, carry):
        w_remote(n).start()
        w_remote(NT + n).start()
        return carry

    lax.fori_loop(0, NT, send_w, 0)
    for g in range(1, G):
        for dx in (1, 3, 2):
            go(ax(g, dx))
    dn_remote = remote(dn_h, dn.at[c], dn_send.at[0], dn_recv.at[0], peer)
    go(dn_remote)

    def forward_tokens(g):
        for dx in (1, 3, 2):
            ax(g, dx).wait_recv()
            for dw in (1, 3, 2):
                go(af(g, dx, dw))

    def wait_tokens(g, dx):
        for dw in (1, 2, 3):
            af(g, dx, dw).wait_recv()

    isq[...] = jnp.zeros_like(isq)
    hsq[...] = jnp.zeros_like(hsq)

    def rs_copy(s, d, g, h):
        return remote(
            rs.at[s, d, g, h], rs.at[s + 1, d, g, h],
            rs_send.at[s, d, g, h], rs_recv.at[s, d, g, h],
            at(xs(1 if d == 0 else -1), c, z, y),
        )

    def ag_copy(d, g, h, hop, block):
        return remote(
            hid.at[d, g, block, h], hid.at[d, g, block, h],
            ag_send.at[d, g, h, hop], ag_recv.at[d, g, h, hop],
            at(xs(1 if d == 0 else -1), c, z, y),
        )

    def rs_stage(g, s):
        rows = slice(g * R, (g + 1) * R)
        blocks = (xs(-s), xs(s))
        if s == 1:
            wait_tokens(g, 1)
            wait_tokens(g, 3)
        if s == 2:
            wait_tokens(g, 2)

        def tile(n, carry):
            if g == 0 and s == 0:
                for t in (n, NT + n):
                    w_local(t).wait()
                    w_remote(t).wait_recv()
            for d in (0, 1):
                p[d, n] = jnp.dot(
                    tok[blocks[d], rows], gu[d * NT + n], preferred_element_type=F32
                )
            return carry

        lax.fori_loop(0, NT, tile, 0)
        for h in (0, 1):
            part = slice(h * H, (h + 1) * H)
            for d in (0, 1):
                if s == 0:
                    rs[0, d, g, h] = p[d, :, part].astype(BF)
                elif s < 3:
                    rs_copy(s - 1, d, g, h).wait_recv()
                    rs[s, d, g, h] = (rs[s, d, g, h].astype(F32) + p[d, :, part]).astype(BF)
                else:
                    rs_copy(2, d, g, h).wait_recv()
                    for n in range(NT):
                        v = rs[3, d, g, h, n].astype(F32) + p[d, n, part]
                        gate, up = v[:, :128], v[:, 128:]
                        hidden = (gate / (1.0 + jnp.exp(-gate)) * up).astype(BF)
                        hid[d, g, blocks[d], h, :, n * 128 : (n + 1) * 128] = hidden
                    go(ag_copy(d, g, h, 0, blocks[d]))
                if s < 3:
                    go(rs_copy(s, d, g, h))

    def ag_block(d, hop):
        return xs(-hop) if d == 0 else xs(hop)

    def ag_wait(g, hop, onward):
        for h in (0, 1):
            for d in (0, 1):
                block = ag_block(d, hop)
                ag_copy(d, g, h, hop, block).wait_recv()
                if onward:
                    go(ag_copy(d, g, h, hop + 1, block))

    def token_squares(g):
        def body(t, carry):
            v = tok[t, g * R : (g + 1) * R].astype(F32)
            v = (v * v).reshape(R // 8, 8, FC).sum(axis=0)
            isq[0] += v[:, :1024]
            isq[1] += v[:, 1024:]
            return carry

        lax.fori_loop(0, NX, body, 0)

    def hidden_squares(g):
        def body(k, carry):
            for d in (0, 1):
                v = hid[d, g, k // 2, k % 2].astype(F32)
                hsq[d] += (v * v).reshape(H // 8, 8, UH).sum(axis=0)
            return carry

        lax.fori_loop(0, 2 * NX, body, 0)

    def own_piece(h):
        return y == 2 * c + h

    def d_copy(g, k, h, other):
        core = 1 - c if other else c
        block = lax.rem(z + k, 4)
        return remote(
            psend.at[g, core, block, h], drecv.at[g, mp],
            d_send.at[g, k, h, other], d_recv.at[g, mp],
            at(x, core, block, 2 * c + h),
        )

    def down(g):
        def tile(q, carry):
            core, col = q // 4, q % 4
            cols = pl.ds(pl.multiple_of(col * 256, 256), 256)
            acc = jnp.dot(
                hid[0, g].reshape(NX * R, UH), dn[core, 0:UH, cols], preferred_element_type=F32
            ) + jnp.dot(
                hid[1, g].reshape(NX * R, UH), dn[core, UH:, cols], preferred_element_type=F32
            )
            psend[g, core, :, :, :, cols] = acc.astype(BF).reshape(NX, 2, H, 256)
            return carry

        lax.fori_loop(0, 8, tile, 0)
        for k in (2, 1, 3, 0):
            for h in (0, 1):
                for other in (1, 0):
                    if k == 0 and other == 0:

                        @pl.when(own_piece(h))
                        def _():
                            drecv[g, mp] = psend[g, c, z, h]

                        @pl.when(jnp.logical_not(own_piece(h)))
                        def _():
                            d_copy(g, k, h, other).start()
                    else:
                        go(d_copy(g, k, h, other))

    def finish(g):
        mine_too = y // 2 == c

        def arrive(src, carry):
            @pl.when(jnp.logical_not(jnp.logical_and(mine_too, src == mp)))
            def _():
                remote(
                    psend.at[g, 0, 0, 0], drecv.at[g, src],
                    d_send.at[g, 0, 0, 0], d_recv.at[g, src], peer,
                ).wait_recv()

            return carry

        lax.fori_loop(0, 16, arrive, 0)
        for q in range(8):
            cols = slice(q * 128, (q + 1) * 128)
            total = drecv[g, 0, :, cols].astype(F32)
            for src in range(1, 16):
                total += drecv[g, src, :, cols].astype(F32)
            out[g * H : (g + 1) * H, cols] = total.astype(BF)

    forward_tokens(0)
    own.wait()
    rs_stage(0, 0)
    forward_tokens(1)
    rs_stage(0, 1)
    forward_tokens(2)
    rs_stage(0, 2)
    forward_tokens(3)
    rs_stage(0, 3)
    token_squares(0)
    for g in range(1, G):
        rs_stage(g, 0)
        ag_wait(g - 1, 0, True)
        rs_stage(g, 1)
        ag_wait(g - 1, 1, True)
        rs_stage(g, 2)
        token_squares(g)
        ag_wait(g - 1, 2, False)
        if g == 1:
            dn_local.wait()
            dn_remote.wait_recv()
        down(g - 1)
        rs_stage(g, 3)
        hidden_squares(g - 1)
        if g >= 2:
            finish(g - 2)
    i_copy = remote(isq.at[1 - c], isq_r, n_send.at[0], n_recv.at[0], peer)
    go(i_copy)
    ag_wait(G - 1, 0, True)
    ag_wait(G - 1, 1, True)
    i_copy.wait_recv()
    inorm[...] = jnp.sqrt(jnp.sum(isq[c] + isq_r[...], axis=0, keepdims=True))
    ag_wait(G - 1, 2, False)
    down(G - 1)
    hidden_squares(G - 1)
    h_copy = remote(hsq, hsq_r, n_send.at[1], n_recv.at[1], peer)
    go(h_copy)
    finish(G - 2)
    h_copy.wait_recv()
    for d in (0, 1):
        hnorm[:, d * UH : (d + 1) * UH] = jnp.sqrt(
            jnp.sum(hsq[d] + hsq_r[d], axis=0, keepdims=True)
        )
    finish(G - 1)

    def sent_w(n, carry):
        w_remote(n).wait_send()
        return carry

    lax.fori_loop(0, 2 * NT, sent_w, 0)
    for g in range(G):
        for h in (0, 1):

            @pl.when(jnp.logical_not(own_piece(h)))
            def _():
                d_copy(g, 0, h, 0).wait_send()

    for copy in sends:
        copy.wait_send()


def main_call(nrm, gu, dn):
    dma = pltpu.SemaphoreType.DMA
    vm = pltpu.VMEM
    anywhere = pl.BlockSpec(memory_space=pl.ANY)
    in_vmem = pl.BlockSpec(memory_space=pltpu.VMEM)
    return pl.pallas_call(
        main_kernel,
        in_specs=[anywhere] * 3,
        out_specs=[in_vmem] * 3,
        out_shape=[
            jax.ShapeDtypeStruct((128, 1024), BF),
            jax.ShapeDtypeStruct((1, 1024), F32),
            jax.ShapeDtypeStruct((1, 1792), F32),
        ],
        scratch_shapes=[
            vm((2 * NT, FC, 256), BF),
            vm((2, 1792, 1024), BF),
            vm((NX, RT, FC), BF),
            vm((4, 2, G, 2, NT, H, 256), BF),
            vm((2, G, NX, 2, H, UH), BF),
            vm((2, NT, R, 256), F32),
            vm((G, 2, NX, 2, H, 1024), BF),
            vm((G, 16, H, 1024), BF),
            vm((2, 8, 1024), F32),
            vm((8, 1024), F32),
            vm((2, 8, UH), F32),
            vm((2, 8, UH), F32),
            dma((2 * NT,)), dma((2 * NT,)), dma((2 * NT,)),
            dma((1,)), dma((1,)), dma((1,)), dma((1,)),
            dma((G, 3)), dma((G, 3)), dma((G, 3, 3)), dma((G, 3, 3)),
            dma((3, 2, G, 2)), dma((3, 2, G, 2)),
            dma((2, G, 2, 3)), dma((2, G, 2, 3)),
            dma((G, 4, 2, 2)), dma((G, 16)),
            dma((2,)), dma((2,)),
        ],
        compiler_params=pltpu.CompilerParams(
            collective_id=0, has_side_effects=True, vmem_limit_bytes=67043328 - 2**20
        ),
    )(nrm, gu, dn)


def on_device(
    tokens, norm_gain, gate_weight, gate_mask, up_weight, up_mask, down_weight, down_mask
):
    gu = mask_gu(gate_weight, gate_mask, up_weight, up_mask)
    dn = mask_down(down_weight, down_mask)
    nrm = norm_call(tokens, norm_gain)
    mixed, inorm, hnorm = main_call(nrm, gu, dn)
    return mixed, inorm.reshape(1024), hnorm.reshape(1792)


def solution(mesh):
    return jax.shard_map(
        on_device,
        mesh=mesh,
        in_specs=(
            P("dp", None), P(), P("dp", "mp"), P("dp", "mp"),
            P("dp", "mp"), P("dp", "mp"), P("mp", "dp"), P("mp", "dp"),
        ),
        out_specs=(P("mp", "dp"), P("dp"), P("mp")),
        check_vma=False,
    )
```

```python
import jax
import jax.numpy as jnp
from jax import lax
from jax.experimental import pallas as pl
from jax.experimental.pallas import tpu as pltpu
from jax.sharding import PartitionSpec as P

MESH = pl.DeviceIdType.MESH
BF = jnp.bfloat16
F32 = jnp.float32

NX = 4
G = 4
U = 8
RT = 256
NT = 7
FC = 2048
UH = 896


def schedule():
    first, second = range(4), range(4, 8)
    plan = []
    for s in range(4):
        plan += [("product", 0, s)] + [("ring", u, s) for u in first]
        if s == 0:
            plan += [("norm", 2), ("norm", 3)]
        if s == 1:
            plan += [("pass", 2), ("pass", 3), ("down_mask", 0)]
        if s == 2:
            plan += [("down_mask", 1)]
    plan += [("squares", 0), ("product", 1, 0)] + [("ring", u, 0) for u in second]
    plan += [("hop", u, 1) for u in first]
    plan += [("product", 1, 1)] + [("ring", u, 1) for u in second]
    plan += [("hop", u, 2) for u in first]
    plan += [("product", 1, 2)] + [("ring", u, 2) for u in second]
    plan += [("down", 0, 2), ("down", 2, 2), ("product", 1, 3)]
    plan += [("ring", u, 3) for u in second]
    plan += [("squares", 1), ("token_norms",)]
    plan += [("hop", u, 1) for u in second]
    plan += [("finish", u) for u in first[:2]]
    plan += [("hop", u, 2) for u in second]
    plan += [("finish", u) for u in first[2:]]
    plan += [("down", u, 1) for u in second]
    plan += [("hidden_norms",)]
    plan += [("finish", u) for u in second]
    return plan


def main_kernel(
    tok_h, gain, gate_h, gmask_h, up_h, umask_h, dn_h, dmask_h,
    out, inorm, hnorm,
    gu, dn, tok, rs, hid, p, psend, drecv, tk, scl, nsend, wt, lhs, e,
    isq, isq_r, hsq, hsq_r,
    t_sem, m_sem, w_loc, w_send, w_recv, dn_loc, dn_send, dn_recv,
    ax_send, ax_recv, af_send, af_recv, rs_send, rs_recv, ag_send, ag_recv,
    d_send, d_recv, n_send, n_recv,
):
    dp, mp = lax.axis_index("dp"), lax.axis_index("mp")
    x, c = dp // 2, dp % 2
    z, y = mp // 4, mp % 4
    sends = []

    def xs(k):
        return lax.rem(x + k + 4, 4)

    def at(xx, cc, zz, yy):
        return (xx * 2 + cc, zz * 4 + yy)

    peer = at(x, 1 - c, z, y)

    def remote(src, dst, ssem, rsem, dev):
        return pltpu.make_async_remote_copy(
            src_ref=src, dst_ref=dst, send_sem=ssem, recv_sem=rsem,
            device_id=dev, device_id_type=MESH,
        )

    def go(copy):
        copy.start()
        sends.append(copy)

    mine = pl.ds(pl.multiple_of(c * 1024, 1024), 1024)

    def t_local(g, h):
        rows = slice(h * 128 + g * 32, h * 128 + g * 32 + 32)
        return pltpu.make_async_copy(tok_h.at[rows], tk.at[g, h], t_sem.at[g, h])

    def w_local(t, q):
        src = (gate_h, up_h)[q].at[:, pl.ds(pl.multiple_of(t * 128, 128), 128)]
        dst = gu.at[t, mine, pl.ds(q * 128, 128)]
        return pltpu.make_async_copy(src, dst, w_loc.at[t, q])

    def w_remote(t):
        tile = gu.at[t, mine]
        return remote(tile, tile, w_send.at[t], w_recv.at[t], peer)

    g_words = pltpu.make_async_copy(gmask_h, wt.at[0:56, 0:1024], m_sem.at[0])
    u_words = pltpu.make_async_copy(umask_h, wt.at[64:120, 0:1024], m_sem.at[1])
    d_words = pltpu.make_async_copy(dmask_h, wt.at[0:32], m_sem.at[2])
    dn_local = pltpu.make_async_copy(dn_h, dn.at[c], dn_loc.at[0])

    def dn_remote(k):
        rows = slice(k * 896, (k + 1) * 896)
        return remote(dn.at[c, rows], dn.at[c, rows], dn_send.at[k], dn_recv.at[k], peer)

    for g in range(2):
        for h in (0, 1):
            t_local(g, h).start()
    g_words.start()
    u_words.start()

    def load(t, carry):
        w_local(t, 0).start()
        w_local(t, 1).start()
        return carry

    lax.fori_loop(0, 2 * NT, load, 0)
    for g in range(2, 4):
        for h in (0, 1):
            t_local(g, h).start()
    dn_local.start()

    barrier = pltpu.get_barrier_semaphore()
    for k in (1, 2, 3):
        pl.semaphore_signal(barrier, inc=1, device_id=at(xs(k), c, z, y), device_id_type=MESH)

    def greet(k, carry):
        other = lax.rem(c * 16 + mp + k, 32)
        pl.semaphore_signal(
            barrier, inc=1, device_id=(x * 2 + other // 16, other % 16), device_id_type=MESH
        )
        return carry

    lax.fori_loop(1, 32, greet, 0)

    k = lax.broadcasted_iota(jnp.int32, (256, 1792), 0)
    col = lax.broadcasted_iota(jnp.int32, (256, 1792), 1)
    e[...] = jnp.where((k % 64 == col // 32) & (k // 64 == (col % 32) // 8), 1.0, 0.0).astype(BF)
    wt[56:64] = jnp.zeros((8, 1792), jnp.int32)
    wt[120:128] = jnp.zeros((8, 1792), jnp.int32)
    wt[32:56, 1024:] = jnp.zeros((24, 768), jnp.int32)
    wt[64:120, 1024:] = jnp.zeros((56, 768), jnp.int32)
    isq[...] = jnp.zeros_like(isq)
    hsq[...] = jnp.zeros_like(hsq)

    def coord(g):
        return y if g % 2 == 0 else z

    def piece(g, w):
        return pl.ds(pl.multiple_of(g * 64 + w * 16, 16), 16)

    def block_cols(b):
        return pl.ds(pl.multiple_of(b * FC, FC), FC)

    def ax(g, dx):
        return remote(
            nsend.at[g, dx - 1], tok.at[x, piece(g, coord(g))],
            ax_send.at[g, dx - 1], ax_recv.at[g, dx - 1], at(xs(dx), c, z, y),
        )

    def af(g, dx, dw):
        src = xs(-dx)
        rows = piece(g, coord(g))
        w = lax.rem(coord(g) + dw, 4)
        dev = at(x, c, z, w) if g % 2 == 0 else at(x, c, w, y)
        return remote(
            tok.at[src, rows], tok.at[src, rows],
            af_send.at[g, dx - 1, dw - 1], af_recv.at[g, dx - 1, dw - 1], dev,
        )

    def normed(g, h, rows, b):
        cols = block_cols(b)
        v = tk[g, h, rows, cols].astype(F32)
        return (v * scl[g, h, rows, 0:1] * gain[:, cols]).astype(BF)

    def norm(g):
        for h in (0, 1):
            t_local(g, h).wait()
        for h in (0, 1):
            for i in (0, 16):
                rows = slice(i, i + 16)
                total = jnp.zeros((16, 512), F32)
                for b in range(16):
                    v = tk[g, h, rows, b * 512 : (b + 1) * 512].astype(F32)
                    total += v * v
                total = jnp.sum(total, axis=1, keepdims=True)
                scale = lax.rsqrt(total * (1.0 / 8192) + 1e-05)
                scl[g, h, rows] = jnp.broadcast_to(scale, (16, 128))
        w = coord(g)
        rows = pl.ds(pl.multiple_of((w // 2) * 16, 16), 16)
        for dx in (1, 3, 2):
            nsend[g, dx - 1] = normed(g, w % 2, rows, xs(dx))
        if g == 0:
            pl.semaphore_wait(barrier, 34)
        for dx in (1, 3, 2):
            go(ax(g, dx))
        for h in (0, 1):
            for i in (0, 1):
                start = g * 64 + i * 32 + h * 16
                tok[x, start : start + 16] = normed(g, h, slice(i * 16, i * 16 + 16), x)

    def pass_on(g):
        for dx in (1, 3, 2):
            ax(g, dx).wait_recv()
            for dw in (1, 3, 2):
                go(af(g, dx, dw))

    def spread_words(at_row, count, both):
        low = lax.broadcasted_iota(jnp.int32, (128, 128), 1) < 64

        def body(r, carry):
            start = pl.multiple_of(r * 128, 128)
            rows = pl.ds(start, 128)
            w = jnp.transpose(wt[:, rows])
            b = [(lax.shift_right_logical(w, 8 * i) & 255).astype(F32) for i in range(4)]
            t = [pltpu.roll(v, 64, 1) for v in b]
            lhs[rows, 0:128] = jnp.where(low, b[0], t[1]).astype(BF)
            lhs[rows, 128:256] = jnp.where(low, b[2], t[3]).astype(BF)
            if both:
                upper = pl.ds(start + 1024, 128)
                lhs[upper, 0:128] = jnp.where(low, t[0], b[1]).astype(BF)
                lhs[upper, 128:256] = jnp.where(low, t[2], b[3]).astype(BF)
            return carry

        lax.fori_loop(at_row, at_row + count, body, 0)

    bit_of = lax.shift_left(1, lax.broadcasted_iota(jnp.int32, (256, 256), 1) % 8)

    def bits(row, pair):
        cols = pl.ds(pl.multiple_of(pair * 256, 256), 256)
        byte = jnp.dot(lhs[pl.ds(row, 256)], e[:, cols], preferred_element_type=F32)
        return (byte.astype(jnp.int32) & bit_of) != 0

    def mask_pair(j, carry):
        for q in (0, 1):
            for i in (0, 1):
                w_local(2 * j + i, q).wait()

        def body(r, carry):
            start = pl.multiple_of(r * 256, 256)
            rows = pl.ds(pl.multiple_of(c * 1024 + start, 256), 256)
            for q in (0, 1):
                keep = bits(pl.multiple_of(q * 1024 + start, 256), j)
                cols = slice(q * 128, (q + 1) * 128)
                for i in (0, 1):
                    v = gu[2 * j + i, rows, cols].astype(F32)
                    v = jnp.where(keep[:, i * 128 : (i + 1) * 128], v, 0.0)
                    gu[2 * j + i, rows, cols] = v.astype(BF)
            return carry

        lax.fori_loop(0, 4, body, 0)
        w_remote(2 * j).start()
        w_remote(2 * j + 1).start()
        return carry

    def down_mask(k):
        if k == 0:
            d_words.wait()
            spread_words(0, 14, False)
            dn_local.wait()

        def body(r, carry):
            start = pl.multiple_of(k * 896 + r * 128, 128)
            rows = pl.ds(start, 128)
            for j in range(4):
                cols = slice(j * 256, (j + 1) * 256)
                byte = jnp.dot(lhs[rows], e[:, cols], preferred_element_type=F32)
                keep = (byte.astype(jnp.int32) & bit_of[:128]) != 0
                v = dn[c, rows, cols].astype(F32)
                dn[c, rows, cols] = jnp.where(keep, v, 0.0).astype(BF)
            return carry

        lax.fori_loop(0, 7, body, 0)
        go(dn_remote(k))

    def rs_copy(s, d, u):
        return remote(
            rs.at[s, d, u], rs.at[s + 1, d, u], rs_send.at[s, d, u], rs_recv.at[s, d, u],
            at(xs(1 if d == 0 else -1), c, z, y),
        )

    def ag_copy(d, u, hop, block):
        return remote(
            hid.at[d, u, block], hid.at[d, u, block],
            ag_send.at[d, u, hop], ag_recv.at[d, u, hop],
            at(xs(1 if d == 0 else -1), c, z, y),
        )

    def product(q, s):
        rows = slice(q * 128, (q + 1) * 128)
        blocks = (xs(-s), xs(s))
        if s in (1, 2):
            for g in (2 * q, 2 * q + 1):
                for dx in ((1, 3), (2,))[s - 1]:
                    for dw in (1, 2, 3):
                        af(g, dx, dw).wait_recv()

        def tile(n, carry):
            if q == 0 and s == 0:
                w_remote(n).wait_recv()
                w_remote(NT + n).wait_recv()
            for d in (0, 1):
                p[s, d, n] = jnp.dot(
                    tok[blocks[d], rows], gu[d * NT + n], preferred_element_type=F32
                )
            return carry

        lax.fori_loop(0, NT, tile, 0)

    def ring(u, s):
        part = slice((u % 4) * 32, (u % 4) * 32 + 32)
        for d in (0, 1):
            if s:
                rs_copy(s - 1, d, u).wait_recv()
            if s == 0:
                rs[0, d, u] = p[0, d, :, part].astype(BF)
            elif s < 3:
                rs[s, d, u] = (rs[s, d, u].astype(F32) + p[s, d, :, part]).astype(BF)
            if s < 3:
                go(rs_copy(s, d, u))
                continue
            block = xs(1) if d == 0 else xs(-1)
            for n in range(NT):
                v = rs[3, d, u, n].astype(F32) + p[3, d, n, part]
                gate, up = v[:, :128], v[:, 128:]
                hidden = (gate / (1.0 + jnp.exp(-gate)) * up).astype(BF)
                hid[d, u, block, :, :, n * 128 : (n + 1) * 128] = hidden.reshape(2, 16, 128)
            go(ag_copy(d, u, 0, block))

    def arrived(u, hop):
        for d in (0, 1):
            block = xs(-hop) if d == 0 else xs(hop)
            ag_copy(d, u, hop, block).wait_recv()
            if hop < 2:
                go(ag_copy(d, u, hop + 1, block))

    def squares(q):
        def body(t, carry):
            rows = pl.ds(pl.multiple_of(q * 128 + (t % 4) * 32, 32), 32)
            v = tok[t // 4, rows].astype(F32)
            v = (v * v).reshape(4, 8, FC).sum(axis=0)
            isq[0] += v[:, :1024]
            isq[1] += v[:, 1024:]
            return carry

        lax.fori_loop(0, 16, body, 0)

    def hidden_squares(u):
        def body(t, carry):
            for d in (0, 1):
                v = hid[d, u, t].reshape(32, UH).astype(F32)
                hsq[d] += (v * v).reshape(4, 8, UH).sum(axis=0)
            return carry

        lax.fori_loop(0, NX, body, 0)

    def d_copy(u, i):
        k, h, other = i // 4, (i // 2) % 2, i % 2
        core = lax.rem(c + other, 2)
        block = lax.rem(z + k, 4)
        return remote(
            psend.at[u, core, block, h], drecv.at[u, mp], d_send.at[u, i], d_recv.at[u, mp],
            at(x, core, block, 2 * c + h),
        )

    def kept_here(i):
        return jnp.logical_and(i // 4 == 0, jnp.logical_and(i % 2 == 0, y == 2 * c + (i // 2) % 2))

    def down(u, count):
        for v in range(u, u + count):
            arrived(v, 2)
        if u == 0:
            for k in (0, 1):
                dn_remote(k).wait_recv()

        def tile(t, carry):
            core, col = t // 4, t % 4
            cols = pl.ds(pl.multiple_of(col * 256, 256), 256)
            acc = sum(
                jnp.dot(
                    hid[d, u : u + count].reshape(count * 128, UH),
                    dn[core, d * UH : (d + 1) * UH, cols],
                    preferred_element_type=F32,
                )
                for d in (0, 1)
            )
            psend[u : u + count, core, :, :, :, cols] = acc.astype(BF).reshape(
                count, NX, 2, 16, 256
            )
            return carry

        lax.fori_loop(0, 8, tile, 0)

        def send(i, carry):
            i = lax.rem(i + 4, 16)
            for v in range(u, u + count):

                @pl.when(jnp.logical_not(kept_here(i)))
                def _():
                    d_copy(v, i).start()

            return carry

        lax.fori_loop(0, 16, send, 0)

        @pl.when(y // 2 == c)
        def _():
            for v in range(u, u + count):
                drecv[v, mp] = psend[v, c, z, y % 2]

        for v in range(u, u + count):
            hidden_squares(v)

    def finish(u):
        def arrive(src, carry):
            @pl.when(jnp.logical_not(jnp.logical_and(y // 2 == c, src == mp)))
            def _():
                remote(
                    psend.at[u, 0, 0, 0], drecv.at[u, src], d_send.at[u, 0], d_recv.at[u, src], peer
                ).wait_recv()

            return carry

        lax.fori_loop(0, 16, arrive, 0)
        for t in range(2):
            cols = slice(t * 512, (t + 1) * 512)
            total = drecv[u, 0, :, cols].astype(F32)
            for src in range(1, 16):
                total += drecv[u, src, :, cols].astype(F32)
            out[u * 16 : (u + 1) * 16, cols] = total.astype(BF)

    def token_norms():
        copy = remote(isq.at[1 - c], isq_r, n_send.at[0], n_recv.at[0], peer)
        go(copy)
        copy.wait_recv()
        inorm[...] = jnp.sqrt(jnp.sum(isq[c] + isq_r[...], axis=0, keepdims=True))

    def hidden_norms():
        copy = remote(hsq, hsq_r, n_send.at[1], n_recv.at[1], peer)
        go(copy)
        copy.wait_recv()
        for d in (0, 1):
            hnorm[:, d * UH : (d + 1) * UH] = jnp.sqrt(
                jnp.sum(hsq[d] + hsq_r[d], axis=0, keepdims=True)
            )

    tasks = dict(
        norm=norm, product=product, ring=ring, hop=lambda u, h: arrived(u, h - 1), down=down,
        finish=finish, squares=squares, token_norms=token_norms, hidden_norms=hidden_norms,
        down_mask=down_mask,
    )
    tasks["pass"] = pass_on

    with jax.named_scope("norm"):
        norm(0)
        norm(1)
    with jax.named_scope("words"):
        g_words.wait()
        u_words.wait()
        spread_words(0, 8, True)
        d_words.start()
    with jax.named_scope("mask"):
        lax.fori_loop(0, 4, mask_pair, 0)
    with jax.named_scope("pass"):
        pass_on(0)
        pass_on(1)
    with jax.named_scope("mask"):
        lax.fori_loop(4, NT, mask_pair, 0)
    for task in schedule():
        with jax.named_scope("_".join(str(v) for v in task)):
            tasks[task[0]](*task[1:])

    with jax.named_scope("sent"):

        def sent_w(n, carry):
            w_remote(n).wait_send()
            return carry

        lax.fori_loop(0, 2 * NT, sent_w, 0)

        def sent_d(i, carry):
            for u in range(U):

                @pl.when(jnp.logical_not(kept_here(i)))
                def _():
                    d_copy(u, i).wait_send()

            return carry

        lax.fori_loop(0, 16, sent_d, 0)
        for copy in sends:
            copy.wait_send()


def main_call(*args):
    dma = pltpu.SemaphoreType.DMA
    vm = pltpu.VMEM
    anywhere = pl.BlockSpec(memory_space=pl.ANY)
    in_vmem = pl.BlockSpec(memory_space=pltpu.VMEM)
    return pl.pallas_call(
        main_kernel,
        in_specs=[anywhere, in_vmem] + [anywhere] * 6,
        out_specs=[in_vmem] * 3,
        out_shape=[
            jax.ShapeDtypeStruct((128, 1024), BF),
            jax.ShapeDtypeStruct((1, 1024), F32),
            jax.ShapeDtypeStruct((1, 1792), F32),
        ],
        scratch_shapes=[
            vm((2 * NT, FC, 256), BF),
            vm((2, 1792, 1024), BF),
            vm((NX, RT, FC), BF),
            vm((4, 2, U, NT, 32, 256), BF),
            vm((2, U, NX, 2, 16, UH), BF),
            vm((4, 2, NT, 128, 256), F32),
            vm((U, 2, NX, 2, 16, 1024), BF),
            vm((U, 16, 16, 1024), BF),
            vm((G, 2, 32, 8192), BF),
            vm((G, 2, 32, 128), F32),
            vm((G, 3, 16, FC), BF),
            vm((128, 1792), jnp.int32),
            vm((2048, 256), BF),
            vm((256, 1792), BF),
            vm((2, 8, 1024), F32),
            vm((8, 1024), F32),
            vm((2, 8, UH), F32),
            vm((2, 8, UH), F32),
            dma((G, 2)), dma((3,)), dma((2 * NT, 2)), dma((2 * NT,)), dma((2 * NT,)),
            dma((1,)), dma((2,)), dma((2,)),
            dma((G, 3)), dma((G, 3)), dma((G, 3, 3)), dma((G, 3, 3)),
            dma((3, 2, U)), dma((3, 2, U)),
            dma((2, U, 3)), dma((2, U, 3)),
            dma((U, 16)), dma((U, 16)),
            dma((2,)), dma((2,)),
        ],
        compiler_params=pltpu.CompilerParams(
            collective_id=0, has_side_effects=True, vmem_limit_bytes=67043328
        ),
    )(*args)


def on_device(
    tokens, norm_gain, gate_weight, gate_mask, up_weight, up_mask, down_weight, down_mask
):
    mixed, inorm, hnorm = main_call(
        tokens, norm_gain.reshape(1, 8192), gate_weight, gate_mask.T, up_weight, up_mask.T,
        down_weight, down_mask.T,
    )
    return mixed, inorm.reshape(1024), hnorm.reshape(1792)


def solution(mesh):
    return jax.shard_map(
        on_device,
        mesh=mesh,
        in_specs=(
            P("dp", None), P(), P("dp", "mp"), P("dp", "mp"),
            P("dp", "mp"), P("dp", "mp"), P("mp", "dp"), P("mp", "dp"),
        ),
        out_specs=(P("mp", "dp"), P("dp"), P("mp")),
        check_vma=False,
    )
```

```python
import jax
import jax.numpy as jnp
from jax import lax
from jax.experimental import pallas as pl
from jax.experimental.pallas import tpu as pltpu
from jax.sharding import PartitionSpec as P

MESH = pl.DeviceIdType.MESH
BF = jnp.bfloat16
F32 = jnp.float32

NX = 4
G = 4
U = 8
RT = 256
NT = 7
FC = 2048
UH = 896


SCHEDULE = (
    ("pass", 0), ("pass", 1), ("product", 0, 0), ("ring", 2, 0), ("ring", 0, 0), ("ring", 1, 0),
    ("ring", 3, 0), ("product", 1, 0), ("ring", 4, 0), ("down_mask", 0), ("pass", 3),
    ("pass", 2), ("product", 0, 1), ("ring", 0, 1), ("product", 0, 2), ("ring", 2, 1),
    ("ring", 1, 1), ("ring", 3, 1), ("ring", 0, 2), ("product", 0, 3), ("product", 1, 1),
    ("ring", 1, 2), ("ring", 0, 3), ("ring", 2, 2), ("ring", 3, 2), ("ring", 1, 3),
    ("hop", 0, 1), ("product", 1, 2), ("ring", 6, 0), ("ring", 4, 1), ("ring", 7, 0),
    ("down_mask", 1), ("ring", 3, 3), ("ring", 2, 3), ("squares", 0), ("ring", 4, 2),
    ("hop", 1, 1), ("product", 1, 3), ("hop", 2, 1), ("hop", 0, 2), ("ring", 4, 3),
    ("hop", 1, 2), ("ring", 6, 1), ("ring", 7, 1), ("ring", 5, 0), ("down", 0, 2), ("hop", 4, 1),
    ("hop", 3, 1), ("ring", 5, 1), ("hop", 4, 2), ("ring", 7, 2), ("hop", 2, 2), ("hop", 3, 2),
    ("ring", 5, 2), ("down", 4, 1), ("ring", 7, 3), ("ring", 6, 2), ("down", 2, 2),
    ("hop", 7, 1), ("ring", 5, 3), ("ring", 6, 3), ("hop", 7, 2), ("hop", 5, 1), ("hop", 6, 1),
    ("down", 7, 1), ("hop", 6, 2), ("finish", 0), ("hop", 5, 2), ("down", 6, 1), ("down", 5, 1),
    ("squares", 1), ("token_norms",), ("finish", 1), ("finish", 6), ("finish", 2), ("finish", 3),
    ("finish", 7), ("finish", 4), ("hidden_norms",), ("finish", 5),
)


def main_kernel(
    tok_h, gain, gate_h, gmask_h, up_h, umask_h, dn_h, dmask_h,
    out, inorm, hnorm,
    gu, dn, tok, rs, hid, p, psend, drecv, tk, scl, nsend, wt, lhs, e,
    isq, isq_r, hsq, hsq_r,
    t_sem, m_sem, w_loc, w_send, w_recv, dn_loc, dn_send, dn_recv,
    ax_send, ax_recv, af_send, af_recv, rs_send, rs_recv, ag_send, ag_recv,
    d_send, d_recv, n_send, n_recv,
):
    dp, mp = lax.axis_index("dp"), lax.axis_index("mp")
    x, c = dp // 2, dp % 2
    z, y = mp // 4, mp % 4
    def xs(k):
        return lax.rem(x + k + 4, 4)

    def at(xx, cc, zz, yy):
        return (xx * 2 + cc, zz * 4 + yy)

    peer = at(x, 1 - c, z, y)

    def remote(src, dst, ssem, rsem, dev):
        return pltpu.make_async_remote_copy(
            src_ref=src, dst_ref=dst, send_sem=ssem, recv_sem=rsem,
            device_id=dev, device_id_type=MESH,
        )

    def came(ref, sem):
        pltpu.make_async_copy(ref, ref, sem).wait()

    mine = pl.ds(pl.multiple_of(c * 1024, 1024), 1024)

    def t_local(g, h):
        rows = slice(h * 128 + g * 32, h * 128 + g * 32 + 32)
        return pltpu.make_async_copy(tok_h.at[rows], tk.at[g, h], t_sem.at[g])

    def w_local(t, q):
        src = (gate_h, up_h)[q].at[:, pl.ds(pl.multiple_of(t * 128, 128), 128)]
        dst = gu.at[t, mine, pl.ds(q * 128, 128)]
        return pltpu.make_async_copy(src, dst, w_loc.at[t // 2])

    def w_remote(t):
        tile = gu.at[t, mine]
        return remote(tile, tile, w_send.at[0], w_recv.at[lax.rem(t, NT)], peer)

    g_words = pltpu.make_async_copy(gmask_h, wt.at[0:56, 0:1024], m_sem.at[0])
    u_words = pltpu.make_async_copy(umask_h, wt.at[64:120, 0:1024], m_sem.at[1])
    d_words = pltpu.make_async_copy(dmask_h, wt.at[0:32], m_sem.at[2])
    dn_local = pltpu.make_async_copy(dn_h, dn.at[c], dn_loc.at[0])

    def dn_remote(k):
        rows = slice(k * 896, (k + 1) * 896)
        return remote(dn.at[c, rows], dn.at[c, rows], dn_send.at[0], dn_recv.at[0], peer)

    g_words.start()
    u_words.start()
    for g in (0, 1):
        for h in (0, 1):
            t_local(g, h).start()

    def load(t, carry):
        w_local(t, 0).start()
        w_local(t, 1).start()
        return carry

    lax.fori_loop(0, 2 * NT, load, 0)
    for g in (2, 3):
        for h in (0, 1):
            t_local(g, h).start()
    dn_local.start()

    barrier = pltpu.get_barrier_semaphore()
    for k in (1, 2, 3):
        pl.semaphore_signal(barrier, inc=1, device_id=at(xs(k), c, z, y), device_id_type=MESH)

    def greet(k, carry):
        other = lax.rem(c * 16 + mp + k, 32)
        pl.semaphore_signal(
            barrier, inc=1, device_id=(x * 2 + other // 16, other % 16), device_id_type=MESH
        )
        return carry

    lax.fori_loop(1, 32, greet, 0)

    k = lax.broadcasted_iota(jnp.int32, (256, 1792), 0)
    col = lax.broadcasted_iota(jnp.int32, (256, 1792), 1)
    e[...] = jnp.where((k % 64 == col // 32) & (k // 64 == (col % 32) // 8), 1.0, 0.0).astype(BF)
    wt[56:64] = jnp.zeros((8, 1792), jnp.int32)
    wt[120:128] = jnp.zeros((8, 1792), jnp.int32)
    wt[32:56, 1024:] = jnp.zeros((24, 768), jnp.int32)
    wt[64:120, 1024:] = jnp.zeros((56, 768), jnp.int32)
    isq[...] = jnp.zeros_like(isq)
    hsq[...] = jnp.zeros_like(hsq)

    def coord(g):
        return y if g % 2 == 0 else z

    def piece(g, w):
        return pl.ds(pl.multiple_of(g * 64 + w * 16, 16), 16)

    def block_cols(b):
        return pl.ds(pl.multiple_of(b * FC, FC), FC)

    def ax(g, dx):
        return remote(
            nsend.at[g, dx - 1], tok.at[x, piece(g, coord(g))],
            ax_send.at[0], ax_recv.at[g], at(xs(dx), c, z, y),
        )

    def af(g, dx, dw):
        src = xs(-dx)
        rows = piece(g, coord(g))
        w = lax.rem(coord(g) + dw, 4)
        dev = at(x, c, z, w) if g % 2 == 0 else at(x, c, w, y)
        return remote(
            tok.at[src, rows], tok.at[src, rows],
            af_send.at[0], af_recv.at[g // 2, dx % 2], dev,
        )

    def normed(g, h, rows, b):
        cols = block_cols(b)
        v = tk[g, h, rows, cols].astype(F32)
        return (v * scl[g, h, rows, 0:1] * gain[:, cols]).astype(BF)

    def norm(g):
        came(tk.at[g], t_sem.at[g])
        for h in (0, 1):
            for i in (0, 16):
                rows = slice(i, i + 16)
                total = jnp.zeros((16, 512), F32)
                for b in range(16):
                    v = tk[g, h, rows, b * 512 : (b + 1) * 512].astype(F32)
                    total += v * v
                total = jnp.sum(total, axis=1, keepdims=True)
                scale = lax.rsqrt(total * (1.0 / 8192) + 1e-05)
                scl[g, h, rows] = jnp.broadcast_to(scale, (16, 128))
        w = coord(g)
        rows = pl.ds(pl.multiple_of((w // 2) * 16, 16), 16)
        for dx in (1, 3, 2):
            nsend[g, dx - 1] = normed(g, w % 2, rows, xs(dx))
        for h in (0, 1):
            for i in (0, 1):
                start = g * 64 + i * 32 + h * 16
                tok[x, start : start + 16] = normed(g, h, slice(i * 16, i * 16 + 16), x)

    def send_tokens(g):
        for dx in (1, 3, 2):
            ax(g, dx).start()

    def pass_on(g):
        came(tok.at[0, 0:48], ax_recv.at[g])
        for dx in (1, 3, 2):
            for dw in (1, 3, 2):
                af(g, dx, dw).start()

    def spread_words(at_row, count, both):
        low = lax.broadcasted_iota(jnp.int32, (128, 128), 1) < 64

        def body(r, carry):
            start = pl.multiple_of(r * 128, 128)
            rows = pl.ds(start, 128)
            w = jnp.transpose(wt[:, rows])
            b = [(lax.shift_right_logical(w, 8 * i) & 255).astype(F32) for i in range(4)]
            t = [pltpu.roll(v, 64, 1) for v in b]
            lhs[rows, 0:128] = jnp.where(low, b[0], t[1]).astype(BF)
            lhs[rows, 128:256] = jnp.where(low, b[2], t[3]).astype(BF)
            if both:
                upper = pl.ds(start + 1024, 128)
                lhs[upper, 0:128] = jnp.where(low, t[0], b[1]).astype(BF)
                lhs[upper, 128:256] = jnp.where(low, t[2], b[3]).astype(BF)
            return carry

        lax.fori_loop(at_row, at_row + count, body, 0)

    bit_of = lax.shift_left(1, lax.broadcasted_iota(jnp.int32, (1, 256), 1) % 8)

    def bits(rows, pair):
        cols = pl.ds(pl.multiple_of(pair * 256, 256), 256)
        byte = jnp.dot(lhs[rows], e[:, cols], preferred_element_type=F32)
        return (byte.astype(jnp.int32) & bit_of) != 0

    def mask_pair(j):
        came(gu.at[pl.ds(2 * j, 2), mine], w_loc.at[j])
        for q in (0, 1):
            keep = bits(slice(q * 1024, (q + 1) * 1024), j)
            cols = slice(q * 128, (q + 1) * 128)
            for i in (0, 1):
                v = gu[2 * j + i, mine, cols].astype(F32)
                v = jnp.where(keep[:, i * 128 : (i + 1) * 128], v, 0.0)
                gu[2 * j + i, mine, cols] = v.astype(BF)

    def swap_pair(j):
        w_remote(2 * j).start()
        w_remote(2 * j + 1).start()

    def mask_and_swap(j, carry):
        mask_pair(j)
        swap_pair(j)
        return carry

    def down_mask(k):
        if k == 0:
            d_words.wait()
            spread_words(0, 14, False)
            dn_local.wait()
        rows = slice(k * 896, (k + 1) * 896)

        def body(j, carry):
            cols = pl.ds(pl.multiple_of(j * 256, 256), 256)
            v = dn[c, rows, cols].astype(F32)
            dn[c, rows, cols] = jnp.where(bits(rows, j), v, 0.0).astype(BF)
            return carry

        lax.fori_loop(0, 4, body, 0)
        dn_remote(k).start()

    def rs_copy(s, d, u):
        return remote(
            rs.at[s, d, u], rs.at[s + 1, d, u], rs_send.at[0], rs_recv.at[s, u],
            at(xs(1 if d == 0 else -1), c, z, y),
        )

    def ag_copy(d, u, hop, block):
        return remote(
            hid.at[d, u, block], hid.at[d, u, block],
            ag_send.at[0], ag_recv.at[u, hop],
            at(xs(1 if d == 0 else -1), c, z, y),
        )

    def product(q, s):
        rows = slice(q * 128, (q + 1) * 128)
        blocks = (xs(-s), xs(s))
        if s == 1:
            came(tok.at[0, 0:192], af_recv.at[q, 1])
        if s == 2:
            came(tok.at[0, 0:96], af_recv.at[q, 0])

        def tile(n, carry):
            if q == 0 and s == 0:
                came(gu.at[0:2, mine], w_recv.at[n])
            for d in (0, 1):
                p[s, d, n] = jnp.dot(
                    tok[blocks[d], rows], gu[d * NT + n], preferred_element_type=F32
                )
            return carry

        lax.fori_loop(0, NT, tile, 0)

    def ring(u, s):
        part = slice((u % 4) * 32, (u % 4) * 32 + 32)
        if s:
            came(rs.at[s, :, u], rs_recv.at[s - 1, u])
        for d in (0, 1):
            if s == 0:
                rs[0, d, u] = p[0, d, :, part].astype(BF)
            elif s < 3:
                rs[s, d, u] = (rs[s, d, u].astype(F32) + p[s, d, :, part]).astype(BF)
            if s < 3:
                rs_copy(s, d, u).start()
                continue
            block = xs(1) if d == 0 else xs(-1)
            for n in range(NT):
                v = rs[3, d, u, n].astype(F32) + p[3, d, n, part]
                gate, up = v[:, :128], v[:, 128:]
                hidden = (gate / (1.0 + jnp.exp(-gate)) * up).astype(BF)
                hid[d, u, block, :, :, n * 128 : (n + 1) * 128] = hidden.reshape(2, 16, 128)
            ag_copy(d, u, 0, block).start()

    def arrived(u, hop):
        came(hid.at[:, u, 0], ag_recv.at[u, hop])
        for d in (0, 1):
            block = xs(-hop) if d == 0 else xs(hop)
            if hop < 2:
                ag_copy(d, u, hop + 1, block).start()

    def squares(q):
        def body(t, carry):
            rows = pl.ds(pl.multiple_of(q * 128 + (t % 4) * 32, 32), 32)
            v = tok[t // 4, rows].astype(F32)
            v = (v * v).reshape(4, 8, FC).sum(axis=0)
            isq[0] += v[:, :1024]
            isq[1] += v[:, 1024:]
            return carry

        lax.fori_loop(0, 16, body, 0)

    def hidden_squares(u):
        def body(t, carry):
            for d in (0, 1):
                v = hid[d, u, t].reshape(32, UH).astype(F32)
                hsq[d] += (v * v).reshape(4, 8, UH).sum(axis=0)
            return carry

        lax.fori_loop(0, NX, body, 0)

    def d_copy(u, i):
        k, h, other = i // 4, (i // 2) % 2, i % 2
        core = lax.rem(c + other, 2)
        block = lax.rem(z + k, 4)
        return remote(
            psend.at[u, core, block, h], drecv.at[u, mp], d_send.at[0], d_recv.at[u],
            at(x, core, block, 2 * c + h),
        )

    def kept_here(i):
        return jnp.logical_and(i // 4 == 0, jnp.logical_and(i % 2 == 0, y == 2 * c + (i // 2) % 2))

    def down(u, count):
        for v in range(u, u + count):
            arrived(v, 2)
        if u == 0:
            came(dn.at[0], dn_recv.at[0])

        def tile(t, carry):
            core, col = t // 2, t % 2
            cols = pl.ds(pl.multiple_of(col * 512, 512), 512)
            acc = sum(
                jnp.dot(
                    hid[d, u : u + count].reshape(count * 128, UH),
                    dn[core, d * UH : (d + 1) * UH, cols],
                    preferred_element_type=F32,
                )
                for d in (0, 1)
            )
            psend[u : u + count, core, :, :, :, cols] = acc.astype(BF).reshape(
                count, NX, 2, 16, 512
            )
            return carry

        lax.fori_loop(0, 4, tile, 0)

        def send(i, carry):
            i = lax.rem(i + 4, 16)
            for v in range(u, u + count):

                @pl.when(jnp.logical_not(kept_here(i)))
                def _():
                    d_copy(v, i).start()

            return carry

        lax.fori_loop(0, 16, send, 0)

        @pl.when(y // 2 == c)
        def _():
            for v in range(u, u + count):
                drecv[v, mp] = psend[v, c, z, y % 2]

        for v in range(u, u + count):
            hidden_squares(v)

    def finish(u):
        here = y // 2 == c

        @pl.when(here)
        def _():
            came(drecv.at[u, 0:15], d_recv.at[u])

        @pl.when(jnp.logical_not(here))
        def _():
            came(drecv.at[u], d_recv.at[u])

        for t in range(2):
            cols = slice(t * 512, (t + 1) * 512)
            total = drecv[u, 0, :, cols].astype(F32)
            for src in range(1, 16):
                total += drecv[u, src, :, cols].astype(F32)
            out[u * 16 : (u + 1) * 16, cols] = total.astype(BF)

    def token_norms():
        copy = remote(isq.at[1 - c], isq_r, n_send.at[0], n_recv.at[0], peer)
        copy.start()
        copy.wait_recv()
        inorm[...] = jnp.sqrt(jnp.sum(isq[c] + isq_r[...], axis=0, keepdims=True))

    def hidden_norms():
        copy = remote(hsq, hsq_r, n_send.at[1], n_recv.at[1], peer)
        copy.start()
        copy.wait_recv()
        for d in (0, 1):
            hnorm[:, d * UH : (d + 1) * UH] = jnp.sqrt(
                jnp.sum(hsq[d] + hsq_r[d], axis=0, keepdims=True)
            )

    tasks = dict(
        product=product, ring=ring, hop=lambda u, h: arrived(u, h - 1), down=down,
        finish=finish, squares=squares, token_norms=token_norms, hidden_norms=hidden_norms,
        down_mask=down_mask,
    )
    tasks["pass"] = pass_on

    with jax.named_scope("words"):
        g_words.wait()
        u_words.wait()
        spread_words(0, 8, True)
        d_words.start()
    with jax.named_scope("norm"):
        norm(0)
        norm(1)
    with jax.named_scope("mask0"):
        mask_pair(0)
    with jax.named_scope("barrier"):
        pl.semaphore_wait(barrier, 34)
    send_tokens(0)
    swap_pair(0)
    send_tokens(1)
    with jax.named_scope("mask"):
        lax.fori_loop(1, NT, mask_and_swap, 0)
    with jax.named_scope("norm"):
        for g in (2, 3):
            norm(g)
            send_tokens(g)
    for task in SCHEDULE:
        with jax.named_scope("_".join(str(v) for v in task)):
            tasks[task[0]](*task[1:])

    with jax.named_scope("sent"):

        came(gu.at[:, mine], w_send.at[0])
        came(dn.at[0], dn_send.at[0])
        came(nsend, ax_send.at[0])
        came(tok.at[0:3, 0:192], af_send.at[0])
        came(rs.at[0:3], rs_send.at[0])
        came(hid.at[:, :, 0:3], ag_send.at[0])
        came(isq.at[0], n_send.at[0])
        came(hsq, n_send.at[1])

        @pl.when(y // 2 == c)
        def _():
            came(drecv.at[:, 0:15], d_send.at[0])

        @pl.when(y // 2 != c)
        def _():
            came(drecv, d_send.at[0])


def main_call(*args):
    dma = pltpu.SemaphoreType.DMA
    vm = pltpu.VMEM
    anywhere = pl.BlockSpec(memory_space=pl.ANY)
    in_vmem = pl.BlockSpec(memory_space=pltpu.VMEM)
    return pl.pallas_call(
        main_kernel,
        in_specs=[anywhere, in_vmem] + [anywhere] * 6,
        out_specs=[in_vmem] * 3,
        out_shape=[
            jax.ShapeDtypeStruct((128, 1024), BF),
            jax.ShapeDtypeStruct((1, 1024), F32),
            jax.ShapeDtypeStruct((1, 1792), F32),
        ],
        scratch_shapes=[
            vm((2 * NT, FC, 256), BF),
            vm((2, 1792, 1024), BF),
            vm((NX, RT, FC), BF),
            vm((4, 2, U, NT, 32, 256), BF),
            vm((2, U, NX, 2, 16, UH), BF),
            vm((4, 2, NT, 128, 256), F32),
            vm((U, 2, NX, 2, 16, 1024), BF),
            vm((U, 16, 16, 1024), BF),
            vm((G, 2, 32, 8192), BF),
            vm((G, 2, 32, 128), F32),
            vm((G, 3, 16, FC), BF),
            vm((128, 1792), jnp.int32),
            vm((2048, 256), BF),
            vm((256, 1792), BF),
            vm((2, 8, 1024), F32),
            vm((8, 1024), F32),
            vm((2, 8, UH), F32),
            vm((2, 8, UH), F32),
            dma((G,)), dma((3,)), dma((NT,)), dma((1,)), dma((NT,)),
            dma((1,)), dma((1,)), dma((1,)),
            dma((1,)), dma((G,)), dma((1,)), dma((2, 2)),
            dma((1,)), dma((3, U)),
            dma((1,)), dma((U, 3)),
            dma((1,)), dma((U,)),
            dma((2,)), dma((2,)),
        ],
        compiler_params=pltpu.CompilerParams(
            collective_id=0, has_side_effects=True, vmem_limit_bytes=67043328
        ),
    )(*args)


def hand_out(mixed, inorm, hnorm, mixed_out, inorm_out, hnorm_out):
    mixed_out[...] = mixed[...]
    inorm_out[...] = inorm[...].reshape(1024)
    hnorm_out[...] = hnorm[...].reshape(1792)


def on_device(
    tokens, norm_gain, gate_weight, gate_mask, up_weight, up_mask, down_weight, down_mask
):
    mixed, inorm, hnorm = main_call(
        tokens, norm_gain.reshape(1, 8192), gate_weight, gate_mask.T, up_weight, up_mask.T,
        down_weight, down_mask.T,
    )
    return pl.pallas_call(
        hand_out,
        out_shape=[
            jax.ShapeDtypeStruct((128, 1024), BF),
            jax.ShapeDtypeStruct((1024,), F32),
            jax.ShapeDtypeStruct((1792,), F32),
        ],
    )(mixed, inorm, hnorm)


def solution(mesh):
    return jax.shard_map(
        on_device,
        mesh=mesh,
        in_specs=(
            P("dp", None), P(), P("dp", "mp"), P("dp", "mp"),
            P("dp", "mp"), P("dp", "mp"), P("mp", "dp"), P("mp", "dp"),
        ),
        out_specs=(P("mp", "dp"), P("dp"), P("mp")),
        check_vma=False,
    )
```

```python
import jax
import jax.numpy as jnp
from jax import lax
from jax.experimental import pallas as pl
from jax.experimental.pallas import tpu as pltpu
from jax.sharding import PartitionSpec as P

MESH = pl.DeviceIdType.MESH
BF = jnp.bfloat16
F32 = jnp.float32

NX = 4
G = 4
U = 8
RT = 256
NT = 7
FC = 2048
UH = 896


LAST = 7

SCHEDULE = (
    ("pass", 0), ("pass", 1), ("product", 0, 0), ("ring", 0, 0), ("ring", 2, 0), ("ring", 3, 0),
    ("pass", 2), ("ring", 1, 0), ("product", 1, 0), ("product", 0, 1), ("ring", 0, 1),
    ("ring", 2, 1), ("down_mask", 0), ("ring", 4, 0), ("pass", 3), ("ring", 1, 1),
    ("ring", 3, 1), ("product", 0, 3), ("product", 0, 2), ("ring", 2, 2), ("ring", 1, 2),
    ("product", 1, 1), ("ring", 3, 2), ("ring", 0, 2), ("ring", 2, 3), ("ring", 3, 3),
    ("ring", 1, 3), ("down_mask", 1), ("ring", 0, 3), ("hop", 2, 1), ("hop", 3, 1),
    ("hop", 0, 1), ("ring", 6, 0), ("hop", 1, 1), ("hop", 3, 2), ("hop", 2, 2),
    ("product", 1, 3), ("ring", 4, 1), ("product", 1, 2), ("squares", 0), ("ring", 5, 0), ("ring", 4, 2),
    ("hop", 0, 2), ("ring", 6, 1), ("down", 2, 2), ("ring", 4, 3), ("hop", 1, 2), ("ring", 5, 1),
    ("ring", 6, 2), ("ring", 5, 2), ("hop", 4, 1), ("ring", 7, 0), ("down", 0, 2),
    ("ring", 5, 3), ("hop", 4, 2), ("ring", 6, 3), ("hop", 5, 1), ("ring", 7, 1), ("down", 4, 1),
    ("hop", 5, 2), ("hop", 6, 1), ("ring", 7, 2), ("down", 5, 1), ("hop", 6, 2), ("ring", 7, 3),
    ("down", 6, 1), ("squares", 1), ("token_norms",), ("finish", 2), ("finish", 3),
    ("finish", 0), ("finish", 1), ("finish", 4), ("down", 7, 1), ("finish", 5), ("finish", 6),
    ("hidden_norms",), ("finish", 7),
)


def main_kernel(
    tok_h, gain, gate_h, gmask_h, up_h, umask_h, dn_h, dmask_h,
    out, inorm, hnorm,
    gu, dn, tok, rs, hid, p, psend, drecv, tk, scl, nsend, wt, lhs, e,
    isq, isq_r, hsq, hsq_r,
    t_sem, m_sem, w_loc, w_send, w_recv, dn_loc, dn_send, dn_recv,
    ax_send, ax_recv, af_send, af_recv, rs_send, rs_recv, ag_send, ag_recv,
    d_send, d_recv, n_send, n_recv,
):
    dp, mp = lax.axis_index("dp"), lax.axis_index("mp")
    x, c = dp // 2, dp % 2
    z, y = mp // 4, mp % 4
    def xs(k):
        return lax.rem(x + k + 4, 4)

    def at(xx, cc, zz, yy):
        return (xx * 2 + cc, zz * 4 + yy)

    peer = at(x, 1 - c, z, y)

    def remote(src, dst, ssem, rsem, dev):
        return pltpu.make_async_remote_copy(
            src_ref=src, dst_ref=dst, send_sem=ssem, recv_sem=rsem,
            device_id=dev, device_id_type=MESH,
        )

    def came(ref, sem):
        pltpu.make_async_copy(ref, ref, sem).wait()

    mine = pl.ds(pl.multiple_of(c * 1024, 1024), 1024)

    def t_local(g, h):
        rows = slice(h * 128 + g * 32, h * 128 + g * 32 + 32)
        return pltpu.make_async_copy(tok_h.at[rows], tk.at[g, h], t_sem.at[g])

    def w_local(t, q):
        src = (gate_h, up_h)[q].at[:, pl.ds(pl.multiple_of(t * 128, 128), 128)]
        dst = gu.at[t, mine, pl.ds(q * 128, 128)]
        return pltpu.make_async_copy(src, dst, w_loc.at[t // 2])

    def w_remote(t):
        tile = gu.at[t, mine]
        return remote(tile, tile, w_send.at[0], w_recv.at[lax.rem(t, NT)], peer)

    g_words = pltpu.make_async_copy(gmask_h, wt.at[0:56, 0:1024], m_sem.at[0])
    u_words = pltpu.make_async_copy(umask_h, wt.at[64:120, 0:1024], m_sem.at[1])
    d_words = pltpu.make_async_copy(dmask_h, wt.at[0:32], m_sem.at[2])
    dn_local = pltpu.make_async_copy(dn_h, dn.at[c], dn_loc.at[0])

    def dn_remote(k):
        rows = slice(k * 896, (k + 1) * 896)
        return remote(dn.at[c, rows], dn.at[c, rows], dn_send.at[0], dn_recv.at[0], peer)

    g_words.start()
    u_words.start()

    barrier = pltpu.get_barrier_semaphore()
    for k in (1, 2, 3):
        pl.semaphore_signal(barrier, inc=1, device_id=at(xs(k), c, z, y), device_id_type=MESH)

    def greet(k, carry):
        other = lax.rem(c * 16 + mp + k, 32)
        pl.semaphore_signal(
            barrier, inc=1, device_id=(x * 2 + other // 16, other % 16), device_id_type=MESH
        )
        return carry

    lax.fori_loop(1, 32, greet, 0)

    for g in (0, 1):
        for h in (0, 1):
            t_local(g, h).start()

    def load(t, carry):
        w_local(t, 0).start()
        w_local(t, 1).start()
        return carry

    lax.fori_loop(0, 2 * NT, load, 0)
    for g in (2, 3):
        for h in (0, 1):
            t_local(g, h).start()
    dn_local.start()

    k = lax.broadcasted_iota(jnp.int32, (256, 128), 0)
    k = (k & 63) * 4 + lax.shift_right_logical(k, 6)
    for j in range(14):
        col = lax.broadcasted_iota(jnp.int32, (256, 128), 1) + j * 128
        here = k == lax.shift_right_logical(col, 3)
        e[:, j * 128 : (j + 1) * 128] = jnp.where(here, 1.0, 0.0).astype(BF)
    wt[56:64] = jnp.zeros((8, 1792), jnp.int32)
    wt[120:128] = jnp.zeros((8, 1792), jnp.int32)
    wt[32:56, 1024:] = jnp.zeros((24, 768), jnp.int32)
    wt[64:120, 1024:] = jnp.zeros((56, 768), jnp.int32)
    isq[...] = jnp.zeros_like(isq)
    hsq[...] = jnp.zeros_like(hsq)

    def coord(g):
        return y if g % 2 == 0 else z

    def piece(g, w):
        return pl.ds(pl.multiple_of(g * 64 + w * 16, 16), 16)

    def block_cols(b):
        return pl.ds(pl.multiple_of(b * FC, FC), FC)

    def ax(g, dx):
        return remote(
            nsend.at[g, dx - 1], tok.at[x, piece(g, coord(g))],
            ax_send.at[0], ax_recv.at[g], at(xs(dx), c, z, y),
        )

    def af(g, dx, dw):
        src = xs(-dx)
        rows = piece(g, coord(g))
        w = lax.rem(coord(g) + dw, 4)
        dev = at(x, c, z, w) if g % 2 == 0 else at(x, c, w, y)
        return remote(
            tok.at[src, rows], tok.at[src, rows],
            af_send.at[0], af_recv.at[g // 2, dx % 2], dev,
        )

    def normed(g, h, rows, b):
        cols = block_cols(b)
        v = tk[g, h, rows, cols].astype(F32)
        return (v * scl[g, h, rows, 0:1] * gain[:, cols]).astype(BF)

    def norm(g):
        came(tk.at[g], t_sem.at[g])
        for h in (0, 1):
            for i in (0, 16):
                rows = slice(i, i + 16)
                total = jnp.zeros((16, 512), F32)
                for b in range(16):
                    v = tk[g, h, rows, b * 512 : (b + 1) * 512].astype(F32)
                    total += v * v
                total = jnp.sum(total, axis=1, keepdims=True)
                scale = lax.rsqrt(total * (1.0 / 8192) + 1e-05)
                scl[g, h, rows] = jnp.broadcast_to(scale, (16, 128))
        w = coord(g)
        rows = pl.ds(pl.multiple_of((w // 2) * 16, 16), 16)
        for dx in (1, 3, 2):
            nsend[g, dx - 1] = normed(g, w % 2, rows, xs(dx))
        for h in (0, 1):
            for i in (0, 1):
                start = g * 64 + i * 32 + h * 16
                tok[x, start : start + 16] = normed(g, h, slice(i * 16, i * 16 + 16), x)

    def send_tokens(g):
        for dx in (1, 3, 2):
            ax(g, dx).start()

    def pass_on(g):
        came(tok.at[0, 0:48], ax_recv.at[g])
        for dx in (1, 3, 2):
            for dw in (1, 3, 2):
                af(g, dx, dw).start()

    def spread_words(at_row, count, both):
        low = lax.broadcasted_iota(jnp.int32, (128, 128), 1) < 64

        def body(r, carry):
            start = pl.multiple_of(r * 128, 128)
            rows = pl.ds(start, 128)
            w = jnp.transpose(wt[:, rows])
            b = [(lax.shift_right_logical(w, 8 * i) & 255).astype(F32) for i in range(4)]
            t = [pltpu.roll(v, 64, 1) for v in b]
            lhs[rows, 0:128] = jnp.where(low, b[0], t[1]).astype(BF)
            lhs[rows, 128:256] = jnp.where(low, b[2], t[3]).astype(BF)
            if both:
                upper = pl.ds(start + 1024, 128)
                lhs[upper, 0:128] = jnp.where(low, t[0], b[1]).astype(BF)
                lhs[upper, 128:256] = jnp.where(low, t[2], b[3]).astype(BF)
            return carry

        lax.fori_loop(at_row, at_row + count, body, 0)

    bit_of = lax.shift_left(1, lax.broadcasted_iota(jnp.int32, (1, 256), 1) % 8)

    def bits(rows, pair):
        cols = pl.ds(pl.multiple_of(pair * 256, 256), 256)
        byte = jnp.dot(lhs[rows], e[:, cols], preferred_element_type=F32)
        return (byte.astype(jnp.int32) & bit_of) != 0

    def mask_pair(j):
        came(gu.at[pl.ds(2 * j, 2), mine], w_loc.at[j])
        for q in (0, 1):
            keep = bits(slice(q * 1024, (q + 1) * 1024), j)
            cols = slice(q * 128, (q + 1) * 128)
            for i in (0, 1):
                v = gu[2 * j + i, mine, cols].astype(F32)
                v = jnp.where(keep[:, i * 128 : (i + 1) * 128], v, 0.0)
                gu[2 * j + i, mine, cols] = v.astype(BF)

    def swap_pair(j):
        w_remote(2 * j).start()
        w_remote(2 * j + 1).start()

    def mask_and_swap(j, carry):
        mask_pair(j)
        swap_pair(j)
        return carry

    def down_mask(k):
        if k == 0:
            d_words.wait()
            spread_words(0, 14, False)
            dn_local.wait()
        rows = slice(k * 896, (k + 1) * 896)

        def body(j, carry):
            cols = pl.ds(pl.multiple_of(j * 256, 256), 256)
            v = dn[c, rows, cols].astype(F32)
            dn[c, rows, cols] = jnp.where(bits(rows, j), v, 0.0).astype(BF)
            return carry

        lax.fori_loop(0, 4, body, 0)
        dn_remote(k).start()

    def rs_copy(s, d, u):
        return remote(
            rs.at[s, d, u], rs.at[s + 1, d, u], rs_send.at[0], rs_recv.at[s, u],
            at(xs(1 if d == 0 else -1), c, z, y),
        )

    def ag_copy(d, u, hop, block):
        return remote(
            hid.at[d, u, block], hid.at[d, u, block],
            ag_send.at[0], ag_recv.at[u, hop],
            at(xs(1 if d == 0 else -1), c, z, y),
        )

    def ag_direct(d, k, block):
        part = hid.at[d, LAST, block]
        dev = at(xs(k if d == 0 else -k), c, z, y)
        return remote(part, part, ag_send.at[0], ag_recv.at[LAST, k - 1], dev)

    def product(q, s):
        rows = slice(q * 128, (q + 1) * 128)
        blocks = (xs(-s), xs(s))
        if s == 1:
            came(tok.at[0, 0:192], af_recv.at[q, 1])
        if s == 2:
            came(tok.at[0, 0:96], af_recv.at[q, 0])

        def tile(n, carry):
            if q == 0 and s == 0:
                came(gu.at[0:2, mine], w_recv.at[n])
            for d in (0, 1):
                p[s, d, n] = jnp.dot(
                    tok[blocks[d], rows], gu[d * NT + n], preferred_element_type=F32
                )
            return carry

        lax.fori_loop(0, NT, tile, 0)

    def ring(u, s):
        part = slice((u % 4) * 32, (u % 4) * 32 + 32)
        if s:
            came(rs.at[s, :, u], rs_recv.at[s - 1, u])
        for d in (0, 1):
            if s == 0:
                rs[0, d, u] = p[0, d, :, part].astype(BF)
            elif s < 3:
                rs[s, d, u] = (rs[s, d, u].astype(F32) + p[s, d, :, part]).astype(BF)
            if s < 3:
                rs_copy(s, d, u).start()
                continue
            block = xs(1) if d == 0 else xs(-1)
            for n in range(NT):
                v = rs[3, d, u, n].astype(F32) + p[3, d, n, part]
                gate, up = v[:, :128], v[:, 128:]
                hidden = (gate / (1.0 + jnp.exp(-gate)) * up).astype(BF)
                hid[d, u, block, :, :, n * 128 : (n + 1) * 128] = hidden.reshape(2, 16, 128)
            if u == LAST:
                for k in (2, 1, 3):
                    ag_direct(d, k, block).start()
            else:
                ag_copy(d, u, 0, block).start()

    def arrived(u, hop):
        came(hid.at[:, u, 0], ag_recv.at[u, hop])
        for d in (0, 1):
            block = xs(-hop) if d == 0 else xs(hop)
            if hop < 2:
                ag_copy(d, u, hop + 1, block).start()

    def squares(q):
        def body(t, carry):
            rows = pl.ds(pl.multiple_of(q * 128 + (t % 4) * 32, 32), 32)
            v = tok[t // 4, rows].astype(F32)
            v = (v * v).reshape(4, 8, FC).sum(axis=0)
            isq[0] += v[:, :1024]
            isq[1] += v[:, 1024:]
            return carry

        lax.fori_loop(0, 16, body, 0)

    def hidden_squares(u):
        def body(t, carry):
            for d in (0, 1):
                v = hid[d, u, t].reshape(32, UH).astype(F32)
                hsq[d] += (v * v).reshape(4, 8, UH).sum(axis=0)
            return carry

        lax.fori_loop(0, NX, body, 0)

    def d_copy(u, i):
        k, h, other = i // 4, (i // 2) % 2, i % 2
        core = lax.rem(c + other, 2)
        block = lax.rem(z + k, 4)
        return remote(
            psend.at[u, core, block, h], drecv.at[u, mp], d_send.at[0], d_recv.at[u],
            at(x, core, block, 2 * c + h),
        )

    def kept_here(i):
        return jnp.logical_and(i // 4 == 0, jnp.logical_and(i % 2 == 0, y == 2 * c + (i // 2) % 2))

    first_down = next(task for task in SCHEDULE if task[0] == "down")

    def down(u, count):
        for v in range(u, u + count):
            for hop in (0, 1) if v == LAST else ():
                came(hid.at[:, v, 0], ag_recv.at[v, hop])
            arrived(v, 2)
        if ("down", u, count) == first_down:
            came(dn.at[0], dn_recv.at[0])

        for other, core in ((1, 1 - c), (0, c)):

            def tile(t, inner, core=core):
                cols = pl.ds(pl.multiple_of(t * 512, 512), 512)
                acc = sum(
                    jnp.dot(
                        hid[d, u : u + count].reshape(count * 128, UH),
                        dn[core, d * UH : (d + 1) * UH, cols],
                        preferred_element_type=F32,
                    )
                    for d in (0, 1)
                )
                acc = acc.astype(BF)
                for i in range(count):
                    part = acc[i * 128 : (i + 1) * 128].reshape(NX, 2, 16, 512)
                    psend[u + i, core, :, :, :, cols] = part
                return inner

            lax.fori_loop(0, 2, tile, 0)

            def send(i, inner, other=other):
                i = lax.rem(i + 2, 8) * 2 + other
                for v in range(u, u + count):

                    @pl.when(jnp.logical_not(kept_here(i)))
                    def _():
                        d_copy(v, i).start()

                return inner

            lax.fori_loop(0, 8, send, 0)

        @pl.when(y // 2 == c)
        def _():
            for v in range(u, u + count):
                drecv[v, mp] = psend[v, c, z, y % 2]

        for v in range(u, u + count):
            hidden_squares(v)

    def finish(u):
        here = y // 2 == c

        @pl.when(here)
        def _():
            came(drecv.at[u, 0:15], d_recv.at[u])

        @pl.when(jnp.logical_not(here))
        def _():
            came(drecv.at[u], d_recv.at[u])

        for t in range(2):
            cols = slice(t * 512, (t + 1) * 512)
            total = drecv[u, 0, :, cols].astype(F32)
            for src in range(1, 16):
                total += drecv[u, src, :, cols].astype(F32)
            out[u * 16 : (u + 1) * 16, cols] = total.astype(BF)

    def token_norms():
        copy = remote(isq.at[1 - c], isq_r, n_send.at[0], n_recv.at[0], peer)
        copy.start()
        copy.wait_recv()
        inorm[...] = jnp.sqrt(jnp.sum(isq[c] + isq_r[...], axis=0, keepdims=True))

    def hidden_norms():
        copy = remote(hsq, hsq_r, n_send.at[1], n_recv.at[1], peer)
        copy.start()
        copy.wait_recv()
        for d in (0, 1):
            hnorm[:, d * UH : (d + 1) * UH] = jnp.sqrt(
                jnp.sum(hsq[d] + hsq_r[d], axis=0, keepdims=True)
            )

    tasks = dict(
        product=product, ring=ring, hop=lambda u, h: arrived(u, h - 1), down=down,
        finish=finish, squares=squares, token_norms=token_norms, hidden_norms=hidden_norms,
        down_mask=down_mask,
    )
    tasks["pass"] = pass_on

    with jax.named_scope("words"):
        g_words.wait()
        u_words.wait()
        spread_words(0, 8, True)
        d_words.start()
    with jax.named_scope("norm"):
        norm(0)
        norm(1)
    with jax.named_scope("mask0"):
        mask_pair(0)
    with jax.named_scope("barrier"):
        pl.semaphore_wait(barrier, 34)
    send_tokens(0)
    swap_pair(0)
    send_tokens(1)
    with jax.named_scope("mask"):
        lax.fori_loop(1, NT, mask_and_swap, 0)
    with jax.named_scope("norm"):
        for g in (2, 3):
            norm(g)
            send_tokens(g)
    for task in SCHEDULE:
        with jax.named_scope("_".join(str(v) for v in task)):
            tasks[task[0]](*task[1:])

    with jax.named_scope("sent"):

        came(gu.at[:, mine], w_send.at[0])
        came(dn.at[0], dn_send.at[0])
        came(nsend, ax_send.at[0])
        came(tok.at[0:3, 0:192], af_send.at[0])
        came(rs.at[0:3], rs_send.at[0])
        came(hid.at[:, :, 0:3], ag_send.at[0])
        came(isq.at[0], n_send.at[0])
        came(hsq, n_send.at[1])

        @pl.when(y // 2 == c)
        def _():
            came(drecv.at[:, 0:15], d_send.at[0])

        @pl.when(y // 2 != c)
        def _():
            came(drecv, d_send.at[0])


def main_call(*args):
    dma = pltpu.SemaphoreType.DMA
    vm = pltpu.VMEM
    anywhere = pl.BlockSpec(memory_space=pl.ANY)
    in_vmem = pl.BlockSpec(memory_space=pltpu.VMEM)
    return pl.pallas_call(
        main_kernel,
        in_specs=[anywhere, in_vmem] + [anywhere] * 6,
        out_specs=[in_vmem] * 3,
        out_shape=[
            jax.ShapeDtypeStruct((128, 1024), BF),
            jax.ShapeDtypeStruct((1, 1024), F32),
            jax.ShapeDtypeStruct((1, 1792), F32),
        ],
        scratch_shapes=[
            vm((2 * NT, FC, 256), BF),
            vm((2, 1792, 1024), BF),
            vm((NX, RT, FC), BF),
            vm((4, 2, U, NT, 32, 256), BF),
            vm((2, U, NX, 2, 16, UH), BF),
            vm((4, 2, NT, 128, 256), F32),
            vm((U, 2, NX, 2, 16, 1024), BF),
            vm((U, 16, 16, 1024), BF),
            vm((G, 2, 32, 8192), BF),
            vm((G, 2, 32, 128), F32),
            vm((G, 3, 16, FC), BF),
            vm((128, 1792), jnp.int32),
            vm((2048, 256), BF),
            vm((256, 1792), BF),
            vm((2, 8, 1024), F32),
            vm((8, 1024), F32),
            vm((2, 8, UH), F32),
            vm((2, 8, UH), F32),
            dma((G,)), dma((3,)), dma((NT,)), dma((1,)), dma((NT,)),
            dma((1,)), dma((1,)), dma((1,)),
            dma((1,)), dma((G,)), dma((1,)), dma((2, 2)),
            dma((1,)), dma((3, U)),
            dma((1,)), dma((U, 3)),
            dma((1,)), dma((U,)),
            dma((2,)), dma((2,)),
        ],
        compiler_params=pltpu.CompilerParams(
            collective_id=0, has_side_effects=True, vmem_limit_bytes=67043328
        ),
    )(*args)


def hand_out(mixed, inorm, hnorm, mixed_out, inorm_out, hnorm_out):
    mixed_out[...] = mixed[...]
    inorm_out[...] = inorm[...].reshape(1024)
    hnorm_out[...] = hnorm[...].reshape(1792)


def on_device(
    tokens, norm_gain, gate_weight, gate_mask, up_weight, up_mask, down_weight, down_mask
):
    mixed, inorm, hnorm = main_call(
        tokens, norm_gain.reshape(1, 8192), gate_weight, gate_mask.T, up_weight, up_mask.T,
        down_weight, down_mask.T,
    )
    return pl.pallas_call(
        hand_out,
        out_shape=[
            jax.ShapeDtypeStruct((128, 1024), BF),
            jax.ShapeDtypeStruct((1024,), F32),
            jax.ShapeDtypeStruct((1792,), F32),
        ],
    )(mixed, inorm, hnorm)


def solution(mesh):
    return jax.shard_map(
        on_device,
        mesh=mesh,
        in_specs=(
            P("dp", None), P(), P("dp", "mp"), P("dp", "mp"),
            P("dp", "mp"), P("dp", "mp"), P("mp", "dp"), P("mp", "dp"),
        ),
        out_specs=(P("mp", "dp"), P("dp"), P("mp")),
        check_vma=False,
    )
```

```python
import jax
import jax.numpy as jnp
from jax import lax
from jax.experimental import pallas as pl
from jax.experimental.pallas import tpu as pltpu
from jax.sharding import PartitionSpec as P

MESH = pl.DeviceIdType.MESH
BF = jnp.bfloat16
F32 = jnp.float32

NX = 4
G = 4
U = 8
RT = 256
NT = 7
FC = 2048
UH = 896


LAST = 7

SCHEDULE = (
    ("pass", 0, 1), ("pass", 1, 1), ("product", 0, 0), ("ring", 0, 0), ("ring", 1, 0),
    ("pass", 0, 0), ("pass", 1, 0), ("product", 0, 1), ("pass", 2, 1), ("pass", 2, 0),
    ("ring", 2, 0), ("ring", 3, 0), ("pass", 3, 1), ("pass", 3, 0), ("ring", 1, 1),
    ("product", 0, 2), ("ring", 2, 1), ("down_mask", 0), ("ring", 0, 1), ("product", 1, 0),
    ("ring", 1, 2), ("ring", 3, 1), ("product", 0, 3), ("ring", 0, 2), ("ring", 1, 3),
    ("ring", 3, 2), ("product", 1, 1), ("ring", 0, 3), ("hop", 1, 1), ("ring", 2, 2),
    ("product", 1, 2), ("squares", 0), ("ring", 4, 0), ("down_mask", 1), ("hop", 1, 2),
    ("ring", 2, 3), ("hop", 0, 1), ("ring", 3, 3), ("ring", 4, 1), ("product", 1, 3),
    ("hop", 0, 2), ("ring", 5, 0), ("hop", 2, 1), ("ring", 6, 0), ("hop", 3, 1), ("ring", 4, 2),
    ("down", 0, 2), ("ring", 5, 1), ("hop", 2, 2), ("hop", 3, 2), ("ring", 4, 3), ("ring", 6, 1),
    ("ring", 5, 2), ("hop", 4, 1), ("ring", 7, 0), ("down", 2, 2), ("ring", 5, 3), ("hop", 4, 2),
    ("ring", 6, 2), ("hop", 5, 1), ("ring", 7, 1), ("down", 4, 1), ("ring", 6, 3), ("hop", 5, 2),
    ("hop", 6, 1), ("ring", 7, 2), ("down", 5, 1), ("hop", 6, 2), ("ring", 7, 3), ("down", 6, 1),
    ("squares", 1), ("finish", 0), ("finish", 1), ("finish", 2), ("finish", 3), ("finish", 4),
    ("down", 7, 1), ("finish", 5), ("finish", 6), ("token_norms",), ("hidden_norms",),
    ("finish", 7),
)


def main_kernel(
    tok_h, gain_h, gate_h, gmask_h, up_h, umask_h, dn_h, dmask_h,
    out, inorm, hnorm,
    gu, dn, tok, rs, hid, p, psend, drecv, tk, scl, nsend, wt, lhs, e,
    isq, isq_r, hsq, hsq_r, gain,
    t_sem, m_sem, w_loc, w_send, w_recv, dn_loc, dn_send, dn_recv,
    ax_send, ax_recv, af_send, af_recv, rs_send, rs_recv, ag_send, ag_recv,
    d_send, d_recv, n_send, n_recv,
):
    dp, mp = lax.axis_index("dp"), lax.axis_index("mp")
    x, c = dp // 2, dp % 2
    z, y = mp // 4, mp % 4
    def xs(k):
        return lax.rem(x + k + 4, 4)

    def at(xx, cc, zz, yy):
        return (xx * 2 + cc, zz * 4 + yy)

    peer = at(x, 1 - c, z, y)

    def remote(src, dst, ssem, rsem, dev):
        return pltpu.make_async_remote_copy(
            src_ref=src, dst_ref=dst, send_sem=ssem, recv_sem=rsem,
            device_id=dev, device_id_type=MESH,
        )

    def came(ref, sem):
        pltpu.make_async_copy(ref, ref, sem).wait()

    mine = pl.ds(pl.multiple_of(c * 1024, 1024), 1024)

    def t_local(g, h):
        rows = slice(h * 128 + g * 32, h * 128 + g * 32 + 32)
        return pltpu.make_async_copy(tok_h.at[rows], tk.at[g, h], t_sem.at[g])

    def w_local(t, q):
        src = (gate_h, up_h)[q].at[:, pl.ds(pl.multiple_of(t * 128, 128), 128)]
        dst = gu.at[t, mine, pl.ds(q * 128, 128)]
        return pltpu.make_async_copy(src, dst, w_loc.at[t // 2])

    def w_remote(t):
        tile = gu.at[t, mine]
        return remote(tile, tile, w_send.at[0], w_recv.at[lax.rem(t, NT)], peer)

    g_words = pltpu.make_async_copy(gmask_h, wt.at[0:56, 0:1024], m_sem.at[0])
    u_words = pltpu.make_async_copy(umask_h, wt.at[64:120, 0:1024], m_sem.at[1])
    d_words = pltpu.make_async_copy(dmask_h, wt.at[0:32], m_sem.at[2])
    gain_copy = pltpu.make_async_copy(gain_h, gain, m_sem.at[3])
    dn_local = pltpu.make_async_copy(dn_h, dn.at[c], dn_loc.at[0])

    def dn_remote(k):
        rows = slice(k * 896, (k + 1) * 896)
        return remote(dn.at[c, rows], dn.at[c, rows], dn_send.at[0], dn_recv.at[0], peer)

    g_words.start()
    u_words.start()
    gain_copy.start()

    barrier = pltpu.get_barrier_semaphore()
    for k in (1, 2, 3):
        pl.semaphore_signal(barrier, inc=1, device_id=at(xs(k), c, z, y), device_id_type=MESH)

    def greet(k, carry):
        other = lax.rem(c * 16 + mp + k, 32)
        pl.semaphore_signal(
            barrier, inc=1, device_id=(x * 2 + other // 16, other % 16), device_id_type=MESH
        )
        return carry

    lax.fori_loop(1, 32, greet, 0)

    for g in (0, 1):
        for h in (0, 1):
            t_local(g, h).start()

    def load(t, carry):
        w_local(t, 0).start()
        w_local(t, 1).start()
        return carry

    lax.fori_loop(0, 2 * NT, load, 0)
    for g in (2, 3):
        for h in (0, 1):
            t_local(g, h).start()
    dn_local.start()

    k = lax.broadcasted_iota(jnp.int32, (256, 128), 0)
    k = (k & 63) * 4 + lax.shift_right_logical(k, 6)
    for j in range(14):
        col = lax.broadcasted_iota(jnp.int32, (256, 128), 1) + j * 128
        here = k == lax.shift_right_logical(col, 3)
        e[:, j * 128 : (j + 1) * 128] = jnp.where(here, 1.0, 0.0).astype(BF)
    wt[56:64] = jnp.zeros((8, 1792), jnp.int32)
    wt[120:128] = jnp.zeros((8, 1792), jnp.int32)
    wt[32:56, 1024:] = jnp.zeros((24, 768), jnp.int32)
    wt[64:120, 1024:] = jnp.zeros((56, 768), jnp.int32)
    isq[...] = jnp.zeros_like(isq)
    hsq[...] = jnp.zeros_like(hsq)

    def coord(g):
        return y if g % 2 == 0 else z

    def piece(g, w):
        return pl.ds(pl.multiple_of(g * 64 + w * 16, 16), 16)

    def block_cols(b):
        return pl.ds(pl.multiple_of(b * FC, FC), FC)

    def ax(g, dx):
        return remote(
            nsend.at[g, dx - 1], tok.at[x, piece(g, coord(g))],
            ax_send.at[0], ax_recv.at[g, dx % 2], at(xs(dx), c, z, y),
        )

    def af(g, dx, dw):
        src = xs(-dx)
        rows = piece(g, coord(g))
        w = lax.rem(coord(g) + dw, 4)
        dev = at(x, c, z, w) if g % 2 == 0 else at(x, c, w, y)
        return remote(
            tok.at[src, rows], tok.at[src, rows],
            af_send.at[0], af_recv.at[g // 2, dx % 2], dev,
        )

    def normed(g, h, rows, b):
        cols = block_cols(b)
        v = tk[g, h, rows, cols].astype(F32)
        return (v * scl[g, h, rows, 0:1] * gain[:, cols]).astype(BF)

    def norm(g):
        came(tk.at[g], t_sem.at[g])
        for h in (0, 1):
            for i in (0, 16):
                rows = slice(i, i + 16)
                total = jnp.zeros((16, 512), F32)
                for b in range(16):
                    v = tk[g, h, rows, b * 512 : (b + 1) * 512].astype(F32)
                    total += v * v
                total = jnp.sum(total, axis=1, keepdims=True)
                scale = lax.rsqrt(total * (1.0 / 8192) + 1e-05)
                scl[g, h, rows] = jnp.broadcast_to(scale, (16, 128))
        w = coord(g)
        rows = pl.ds(pl.multiple_of((w // 2) * 16, 16), 16)
        for dx in (1, 3, 2):
            nsend[g, dx - 1] = normed(g, w % 2, rows, xs(dx))
        for h in (0, 1):
            for i in (0, 1):
                start = g * 64 + i * 32 + h * 16
                tok[x, start : start + 16] = normed(g, h, slice(i * 16, i * 16 + 16), x)

    def send_tokens(g, near):
        for dx in (1, 3) if near else (2,):
            ax(g, dx).start()

    def pass_on(g, near):
        came(tok.at[0, 0 : 32 if near else 16], ax_recv.at[g, near])
        for dx in (1, 3) if near else (2,):
            for dw in (1, 3, 2):
                af(g, dx, dw).start()

    def spread_words(at_row, count, both):
        low = lax.broadcasted_iota(jnp.int32, (128, 128), 1) < 64

        def body(r, carry):
            start = pl.multiple_of(r * 128, 128)
            rows = pl.ds(start, 128)
            w = jnp.transpose(wt[:, rows])
            t = pltpu.roll(w, 64, 1)

            def byte_pair(at, below, above, bit):
                below = lax.shift_right_logical(below, bit)
                above = lax.shift_right_logical(above, bit + 8)
                value = jnp.where(low, below, above) & 255
                lhs[at, bit * 8 : bit * 8 + 128] = value.astype(F32).astype(BF)

            for bit in (0, 16):
                byte_pair(rows, w, t, bit)
                if both:
                    byte_pair(pl.ds(start + 1024, 128), t, w, bit)
            return carry

        lax.fori_loop(at_row, at_row + count, body, 0)

    bit_of = lax.shift_left(1, lax.broadcasted_iota(jnp.int32, (1, 256), 1) % 8)

    def bits(rows, pair):
        cols = pl.ds(pl.multiple_of(pair * 256, 256), 256)
        byte = jnp.dot(lhs[rows], e[:, cols], preferred_element_type=F32)
        return (byte.astype(jnp.int32) & bit_of) != 0

    def mask_pair(j):
        came(gu.at[pl.ds(2 * j, 2), mine], w_loc.at[j])
        for q in (0, 1):
            keep = bits(slice(q * 1024, (q + 1) * 1024), j)
            cols = slice(q * 128, (q + 1) * 128)
            for i in (0, 1):
                v = gu[2 * j + i, mine, cols].astype(F32)
                v = jnp.where(keep[:, i * 128 : (i + 1) * 128], v, 0.0)
                gu[2 * j + i, mine, cols] = v.astype(BF)

    def swap_pair(j):
        w_remote(2 * j).start()
        w_remote(2 * j + 1).start()

    def mask_and_swap(j, carry):
        mask_pair(j)
        swap_pair(j)
        return carry

    def down_mask(k):
        if k == 0:
            d_words.wait()
            spread_words(0, 14, False)
            dn_local.wait()
        rows = slice(k * 896, (k + 1) * 896)

        def body(j, carry):
            cols = pl.ds(pl.multiple_of(j * 256, 256), 256)
            v = dn[c, rows, cols].astype(F32)
            dn[c, rows, cols] = jnp.where(bits(rows, j), v, 0.0).astype(BF)
            return carry

        lax.fori_loop(0, 4, body, 0)
        dn_remote(k).start()

    def rs_copy(s, d, u):
        return remote(
            rs.at[s, d, u], rs.at[s + 1, d, u], rs_send.at[0], rs_recv.at[s, u],
            at(xs(1 if d == 0 else -1), c, z, y),
        )

    def ag_copy(d, u, hop, block):
        return remote(
            hid.at[d, u, block], hid.at[d, u, block],
            ag_send.at[0], ag_recv.at[u, hop],
            at(xs(1 if d == 0 else -1), c, z, y),
        )

    def ag_direct(d, k, block):
        part = hid.at[d, LAST, block]
        dev = at(xs(k if d == 0 else -k), c, z, y)
        return remote(part, part, ag_send.at[0], ag_recv.at[LAST, k - 1], dev)

    def product(q, s):
        rows = slice(q * 128, (q + 1) * 128)
        blocks = (xs(-s), xs(s))
        if s == 1:
            came(tok.at[0, 0:192], af_recv.at[q, 1])
        if s == 2:
            came(tok.at[0, 0:96], af_recv.at[q, 0])

        def tile(n, carry):
            if q == 0 and s == 0:
                came(gu.at[0:2, mine], w_recv.at[n])
            for d in (0, 1):
                p[s, d, n] = jnp.dot(
                    tok[blocks[d], rows], gu[d * NT + n], preferred_element_type=F32
                )
            return carry

        lax.fori_loop(0, NT, tile, 0)

    def ring(u, s):
        part = slice((u % 4) * 32, (u % 4) * 32 + 32)
        if s:
            came(rs.at[s, :, u], rs_recv.at[s - 1, u])
        for d in (0, 1):
            if s == 0:
                rs[0, d, u] = p[0, d, :, part].astype(BF)
            elif s < 3:
                rs[s, d, u] = (rs[s, d, u].astype(F32) + p[s, d, :, part]).astype(BF)
            if s < 3:
                rs_copy(s, d, u).start()
                continue
            block = xs(1) if d == 0 else xs(-1)
            for n in range(NT):
                v = rs[3, d, u, n].astype(F32) + p[3, d, n, part]
                gate, up = v[:, :128], v[:, 128:]
                hidden = (gate / (1.0 + jnp.exp(-gate)) * up).astype(BF)
                hid[d, u, block, :, :, n * 128 : (n + 1) * 128] = hidden.reshape(2, 16, 128)
            if u == LAST:
                for k in (2, 1, 3):
                    ag_direct(d, k, block).start()
            else:
                ag_copy(d, u, 0, block).start()

    def arrived(u, hop):
        came(hid.at[:, u, 0], ag_recv.at[u, hop])
        for d in (0, 1):
            block = xs(-hop) if d == 0 else xs(hop)
            if hop < 2:
                ag_copy(d, u, hop + 1, block).start()

    def squares(q):
        def body(t, carry):
            rows = pl.ds(pl.multiple_of(q * 128 + (t % 4) * 32, 32), 32)
            v = tok[t // 4, rows].astype(F32)
            v = (v * v).reshape(4, 8, FC).sum(axis=0)
            isq[0] += v[:, :1024]
            isq[1] += v[:, 1024:]
            return carry

        lax.fori_loop(0, 16, body, 0)

    def hidden_squares(u):
        def body(t, carry):
            for d in (0, 1):
                v = hid[d, u, t].reshape(32, UH).astype(F32)
                hsq[d] += (v * v).reshape(4, 8, UH).sum(axis=0)
            return carry

        lax.fori_loop(0, NX, body, 0)

    def d_copy(u, i):
        k, h, other = i // 4, (i // 2) % 2, i % 2
        core = lax.rem(c + other, 2)
        block = lax.rem(z + k, 4)
        return remote(
            psend.at[u, core, block, h], drecv.at[u, mp], d_send.at[0], d_recv.at[u],
            at(x, core, block, 2 * c + h),
        )

    def kept_here(i):
        return jnp.logical_and(i // 4 == 0, jnp.logical_and(i % 2 == 0, y == 2 * c + (i // 2) % 2))

    first_down = next(task for task in SCHEDULE if task[0] == "down")

    def down(u, count):
        for v in range(u, u + count):
            for hop in (0, 1) if v == LAST else ():
                came(hid.at[:, v, 0], ag_recv.at[v, hop])
            arrived(v, 2)
        if ("down", u, count) == first_down:
            came(dn.at[0], dn_recv.at[0])

        for other, core in ((1, 1 - c), (0, c)):

            def tile(t, inner, core=core):
                cols = pl.ds(pl.multiple_of(t * 512, 512), 512)
                acc = sum(
                    jnp.dot(
                        hid[d, u : u + count].reshape(count * 128, UH),
                        dn[core, d * UH : (d + 1) * UH, cols],
                        preferred_element_type=F32,
                    )
                    for d in (0, 1)
                )
                acc = acc.astype(BF)
                for i in range(count):
                    part = acc[i * 128 : (i + 1) * 128].reshape(NX, 2, 16, 512)
                    psend[u + i, core, :, :, :, cols] = part
                return inner

            lax.fori_loop(0, 2, tile, 0)

            def send(i, inner, other=other):
                i = lax.rem(i + 2, 8) * 2 + other
                for v in range(u, u + count):

                    @pl.when(jnp.logical_not(kept_here(i)))
                    def _():
                        d_copy(v, i).start()

                return inner

            lax.fori_loop(0, 8, send, 0)

        @pl.when(y // 2 == c)
        def _():
            for v in range(u, u + count):
                drecv[v, mp] = psend[v, c, z, y % 2]

        for v in range(u, u + count):
            hidden_squares(v)

    def finish(u):
        here = y // 2 == c

        @pl.when(here)
        def _():
            came(drecv.at[u, 0:15], d_recv.at[u])

        @pl.when(jnp.logical_not(here))
        def _():
            came(drecv.at[u], d_recv.at[u])

        for t in range(2):
            cols = slice(t * 512, (t + 1) * 512)
            total = drecv[u, 0, :, cols].astype(F32)
            for src in range(1, 16):
                total += drecv[u, src, :, cols].astype(F32)
            out[u * 16 : (u + 1) * 16, cols] = total.astype(BF)

    def token_norms():
        copy = remote(isq.at[1 - c], isq_r, n_send.at[0], n_recv.at[0], peer)
        copy.start()
        copy.wait_recv()
        inorm[...] = jnp.sqrt(jnp.sum(isq[c] + isq_r[...], axis=0, keepdims=True))

    def hidden_norms():
        copy = remote(hsq, hsq_r, n_send.at[1], n_recv.at[1], peer)
        copy.start()
        copy.wait_recv()
        for d in (0, 1):
            hnorm[:, d * UH : (d + 1) * UH] = jnp.sqrt(
                jnp.sum(hsq[d] + hsq_r[d], axis=0, keepdims=True)
            )

    tasks = dict(
        product=product, ring=ring, hop=lambda u, h: arrived(u, h - 1), down=down,
        finish=finish, squares=squares, token_norms=token_norms, hidden_norms=hidden_norms,
        down_mask=down_mask,
    )
    tasks["pass"] = pass_on

    with jax.named_scope("words"):
        g_words.wait()
        u_words.wait()
        spread_words(0, 8, True)
        d_words.start()
    with jax.named_scope("mask0"):
        mask_pair(0)
    with jax.named_scope("barrier"):
        pl.semaphore_wait(barrier, 34)
    swap_pair(0)
    with jax.named_scope("norm"):
        gain_copy.wait()
        norm(0)
        send_tokens(0, 1)
    with jax.named_scope("mask"):
        mask_and_swap(1, 0)
    with jax.named_scope("norm"):
        norm(1)
        send_tokens(1, 1)
        send_tokens(0, 0)
        send_tokens(1, 0)
    with jax.named_scope("mask"):
        lax.fori_loop(2, NT, mask_and_swap, 0)
    with jax.named_scope("norm"):
        for g in (2, 3):
            norm(g)
            send_tokens(g, 1)
            send_tokens(g, 0)
    for task in SCHEDULE:
        with jax.named_scope("_".join(str(v) for v in task)):
            tasks[task[0]](*task[1:])

    with jax.named_scope("sent"):

        came(gu.at[:, mine], w_send.at[0])
        came(dn.at[0], dn_send.at[0])
        came(nsend, ax_send.at[0])
        came(tok.at[0:3, 0:192], af_send.at[0])
        came(rs.at[0:3], rs_send.at[0])
        came(hid.at[:, :, 0:3], ag_send.at[0])
        came(isq.at[0], n_send.at[0])
        came(hsq, n_send.at[1])

        @pl.when(y // 2 == c)
        def _():
            came(drecv.at[:, 0:15], d_send.at[0])

        @pl.when(y // 2 != c)
        def _():
            came(drecv, d_send.at[0])


def main_call(*args):
    dma = pltpu.SemaphoreType.DMA
    vm = pltpu.VMEM
    anywhere = pl.BlockSpec(memory_space=pl.ANY)
    in_vmem = pl.BlockSpec(memory_space=pltpu.VMEM)
    return pl.pallas_call(
        main_kernel,
        in_specs=[anywhere] * 8,
        out_specs=[in_vmem] * 3,
        out_shape=[
            jax.ShapeDtypeStruct((128, 1024), BF),
            jax.ShapeDtypeStruct((1, 1024), F32),
            jax.ShapeDtypeStruct((1, 1792), F32),
        ],
        scratch_shapes=[
            vm((2 * NT, FC, 256), BF),
            vm((2, 1792, 1024), BF),
            vm((NX, RT, FC), BF),
            vm((4, 2, U, NT, 32, 256), BF),
            vm((2, U, NX, 2, 16, UH), BF),
            vm((4, 2, NT, 128, 256), F32),
            vm((U, 2, NX, 2, 16, 1024), BF),
            vm((U, 16, 16, 1024), BF),
            vm((G, 2, 32, 8192), BF),
            vm((G, 2, 32, 128), F32),
            vm((G, 3, 16, FC), BF),
            vm((128, 1792), jnp.int32),
            vm((2048, 256), BF),
            vm((256, 1792), BF),
            vm((2, 8, 1024), F32),
            vm((8, 1024), F32),
            vm((2, 8, UH), F32),
            vm((2, 8, UH), F32),
            vm((1, 8192), F32),
            dma((G,)), dma((4,)), dma((NT,)), dma((1,)), dma((NT,)),
            dma((1,)), dma((1,)), dma((1,)),
            dma((1,)), dma((G, 2)), dma((1,)), dma((2, 2)),
            dma((1,)), dma((3, U)),
            dma((1,)), dma((U, 3)),
            dma((1,)), dma((U,)),
            dma((2,)), dma((2,)),
        ],
        compiler_params=pltpu.CompilerParams(
            collective_id=0, has_side_effects=True, vmem_limit_bytes=67043328
        ),
    )(*args)


def hand_out(mixed, inorm, hnorm, mixed_out, inorm_out, hnorm_out):
    mixed_out[...] = mixed[...]
    inorm_out[...] = inorm[...].reshape(1024)
    hnorm_out[...] = hnorm[...].reshape(1792)


def on_device(
    tokens, norm_gain, gate_weight, gate_mask, up_weight, up_mask, down_weight, down_mask
):
    mixed, inorm, hnorm = main_call(
        tokens, norm_gain.reshape(1, 8192), gate_weight, gate_mask.T, up_weight, up_mask.T,
        down_weight, down_mask.T,
    )
    return pl.pallas_call(
        hand_out,
        out_shape=[
            jax.ShapeDtypeStruct((128, 1024), BF),
            jax.ShapeDtypeStruct((1024,), F32),
            jax.ShapeDtypeStruct((1792,), F32),
        ],
    )(mixed, inorm, hnorm)


def solution(mesh):
    return jax.shard_map(
        on_device,
        mesh=mesh,
        in_specs=(
            P("dp", None), P(), P("dp", "mp"), P("dp", "mp"),
            P("dp", "mp"), P("dp", "mp"), P("mp", "dp"), P("mp", "dp"),
        ),
        out_specs=(P("mp", "dp"), P("dp"), P("mp")),
        check_vma=False,
    )
```

```python
import jax
import jax.numpy as jnp
from jax import lax
from jax.experimental import pallas as pl
from jax.experimental.pallas import tpu as pltpu
from jax.sharding import PartitionSpec as P

MESH = pl.DeviceIdType.MESH
BF = jnp.bfloat16
F32 = jnp.float32

NX = 4
G = 4
U = 8
RT = 256
NT = 7
FC = 2048
UH = 896


LAST = 7

SCHEDULE = (
    ("pass", 0, 1), ("pass", 1, 1), ("product", 0, 0), ("ring", 2, 0), ("ring", 0, 0),
    ("ring", 1, 0), ("ring", 3, 0), ("pass", 0, 0), ("pass", 1, 0), ("product", 0, 1),
    ("pass", 3, 1), ("pass", 3, 0), ("down_mask", 0), ("ring", 0, 1), ("ring", 1, 1),
    ("ring", 3, 1), ("pass", 2, 1), ("pass", 2, 0), ("product", 0, 2), ("ring", 0, 2),
    ("ring", 1, 2), ("ring", 2, 1), ("product", 0, 3), ("product", 1, 0), ("ring", 3, 2),
    ("ring", 1, 3), ("ring", 2, 2), ("ring", 0, 3), ("product", 1, 1), ("ring", 3, 3),
    ("down_mask", 1), ("ring", 4, 0), ("hop", 1, 1), ("hop", 0, 1), ("ring", 2, 3),
    ("ring", 4, 1), ("hop", 1, 2), ("hop", 0, 2), ("hop", 2, 1), ("ring", 6, 0), ("hop", 3, 1),
    ("product", 1, 3), ("product", 1, 2), ("squares", 0), ("ring", 4, 2), ("ring", 5, 0),
    ("down", 0, 2), ("hop", 3, 2), ("ring", 6, 1), ("ring", 4, 3), ("hop", 2, 2), ("ring", 5, 1),
    ("ring", 6, 2), ("hop", 4, 1), ("ring", 7, 0), ("down", 2, 2), ("ring", 6, 3), ("hop", 4, 2),
    ("ring", 5, 2), ("hop", 6, 1), ("ring", 7, 1), ("down", 4, 1), ("ring", 5, 3), ("hop", 6, 2),
    ("hop", 5, 1), ("ring", 7, 2), ("down", 6, 1), ("hop", 5, 2), ("ring", 7, 3), ("down", 5, 1),
    ("squares", 1), ("finish", 0), ("finish", 1), ("finish", 2), ("finish", 3), ("finish", 4),
    ("down", 7, 1), ("finish", 6), ("finish", 5), ("token_norms",), ("hidden_norms",),
    ("finish", 7),
)


def main_kernel(
    tok_h, gain_h, gate_h, gmask_h, up_h, umask_h, dn_h, dmask_h,
    out, inorm, hnorm,
    gu, dn, tok, rs, hid, p, psend, drecv, tk, scl, nsend, wt, lhs, e,
    isq, isq_r, hsq, hsq_r, gain,
    t_sem, m_sem, w_loc, w_send, w_recv, dn_loc, dn_send, dn_recv,
    ax_send, ax_recv, af_send, af_recv, rs_send, rs_recv, ag_send, ag_recv,
    d_send, d_recv, n_send, n_recv,
):
    dp, mp = lax.axis_index("dp"), lax.axis_index("mp")
    x, c = dp // 2, dp % 2
    z, y = mp // 4, mp % 4
    def xs(k):
        return lax.rem(x + k + 4, 4)

    def at(xx, cc, zz, yy):
        return (xx * 2 + cc, zz * 4 + yy)

    peer = at(x, 1 - c, z, y)

    def remote(src, dst, ssem, rsem, dev):
        return pltpu.make_async_remote_copy(
            src_ref=src, dst_ref=dst, send_sem=ssem, recv_sem=rsem,
            device_id=dev, device_id_type=MESH,
        )

    def came(ref, sem):
        pltpu.make_async_copy(ref, ref, sem).wait()

    mine = pl.ds(pl.multiple_of(c * 1024, 1024), 1024)

    def t_local(g, h):
        rows = slice(h * 128 + g * 32, h * 128 + g * 32 + 32)
        return pltpu.make_async_copy(tok_h.at[rows], tk.at[g, h], t_sem.at[g])

    def w_local(t, q):
        src = (gate_h, up_h)[q].at[:, pl.ds(pl.multiple_of(t * 128, 128), 128)]
        dst = gu.at[t, mine, pl.ds(q * 128, 128)]
        return pltpu.make_async_copy(src, dst, w_loc.at[t // 2])

    def w_remote(t):
        tile = gu.at[t, mine]
        return remote(tile, tile, w_send.at[0], w_recv.at[lax.rem(t, NT)], peer)

    g_words = pltpu.make_async_copy(gmask_h, wt.at[0:56, 0:1024], m_sem.at[0])
    u_words = pltpu.make_async_copy(umask_h, wt.at[64:120, 0:1024], m_sem.at[1])
    d_words = pltpu.make_async_copy(dmask_h, wt.at[0:32], m_sem.at[2])
    gain_copy = pltpu.make_async_copy(gain_h, gain, m_sem.at[3])
    dn_local = pltpu.make_async_copy(dn_h, dn.at[c], dn_loc.at[0])

    def dn_remote(k):
        rows = slice(k * 896, (k + 1) * 896)
        return remote(dn.at[c, rows], dn.at[c, rows], dn_send.at[0], dn_recv.at[0], peer)

    g_words.start()
    u_words.start()
    gain_copy.start()

    barrier = pltpu.get_barrier_semaphore()
    for k in (1, 2, 3):
        pl.semaphore_signal(barrier, inc=1, device_id=at(xs(k), c, z, y), device_id_type=MESH)

    def greet(k, carry):
        other = lax.rem(c * 16 + mp + k, 32)
        pl.semaphore_signal(
            barrier, inc=1, device_id=(x * 2 + other // 16, other % 16), device_id_type=MESH
        )
        return carry

    lax.fori_loop(1, 32, greet, 0)

    for g in (0, 1):
        for h in (0, 1):
            t_local(g, h).start()

    def load(t, carry):
        w_local(t, 0).start()
        w_local(t, 1).start()
        return carry

    lax.fori_loop(0, 2 * NT, load, 0)
    for g in (2, 3):
        for h in (0, 1):
            t_local(g, h).start()
    dn_local.start()

    k = lax.broadcasted_iota(jnp.int32, (256, 128), 0)
    k = (k & 63) * 4 + lax.shift_right_logical(k, 6)
    for j in range(14):
        col = lax.broadcasted_iota(jnp.int32, (256, 128), 1) + j * 128
        here = k == lax.shift_right_logical(col, 3)
        e[:, j * 128 : (j + 1) * 128] = jnp.where(here, 1.0, 0.0).astype(BF)
    wt[56:64] = jnp.zeros((8, 1792), jnp.int32)
    wt[120:128] = jnp.zeros((8, 1792), jnp.int32)
    wt[32:56, 1024:] = jnp.zeros((24, 768), jnp.int32)
    wt[64:120, 1024:] = jnp.zeros((56, 768), jnp.int32)
    isq[...] = jnp.zeros_like(isq)
    hsq[...] = jnp.zeros_like(hsq)

    def coord(g):
        return y if g % 2 == 0 else z

    def piece(g, w):
        return pl.ds(pl.multiple_of(g * 64 + w * 16, 16), 16)

    def block_cols(b):
        return pl.ds(pl.multiple_of(b * FC, FC), FC)

    def ax(g, dx):
        return remote(
            nsend.at[g, dx - 1], tok.at[x, piece(g, coord(g))],
            ax_send.at[0], ax_recv.at[g, dx % 2], at(xs(dx), c, z, y),
        )

    def af(g, dx, dw):
        src = xs(-dx)
        rows = piece(g, coord(g))
        w = lax.rem(coord(g) + dw, 4)
        dev = at(x, c, z, w) if g % 2 == 0 else at(x, c, w, y)
        return remote(
            tok.at[src, rows], tok.at[src, rows],
            af_send.at[0], af_recv.at[g // 2, dx % 2], dev,
        )

    def normed(g, h, rows, b):
        cols = block_cols(b)
        v = tk[g, h, rows, cols].astype(F32)
        return (v * scl[g, h, rows, 0:1] * gain[:, cols]).astype(BF)

    def norm(g):
        came(tk.at[g], t_sem.at[g])
        for h in (0, 1):
            for i in (0, 16):
                rows = slice(i, i + 16)
                total = jnp.zeros((16, 512), F32)
                for b in range(16):
                    v = tk[g, h, rows, b * 512 : (b + 1) * 512].astype(F32)
                    total += v * v
                total = jnp.sum(total, axis=1, keepdims=True)
                scale = lax.rsqrt(total * (1.0 / 8192) + 1e-05)
                scl[g, h, rows] = jnp.broadcast_to(scale, (16, 128))
        w = coord(g)
        rows = pl.ds(pl.multiple_of((w // 2) * 16, 16), 16)
        for dx in (1, 3, 2):
            nsend[g, dx - 1] = normed(g, w % 2, rows, xs(dx))
        for h in (0, 1):
            for i in (0, 1):
                start = g * 64 + i * 32 + h * 16
                tok[x, start : start + 16] = normed(g, h, slice(i * 16, i * 16 + 16), x)

    def send_tokens(g, near):
        for dx in (1, 3) if near else (2,):
            ax(g, dx).start()

    def pass_on(g, near):
        came(tok.at[0, 0 : 32 if near else 16], ax_recv.at[g, near])
        for dx in (1, 3) if near else (2,):
            for dw in (1, 3, 2):
                af(g, dx, dw).start()

    def spread_words(at_row, count, both):
        low = lax.broadcasted_iota(jnp.int32, (128, 128), 1) < 64

        def body(r, carry):
            start = pl.multiple_of(r * 128, 128)
            rows = pl.ds(start, 128)
            w = jnp.transpose(wt[:, rows])
            t = pltpu.roll(w, 64, 1)

            def byte_pair(at, below, above, bit):
                below = lax.shift_right_logical(below, bit)
                above = lax.shift_right_logical(above, bit + 8)
                value = jnp.where(low, below, above) & 255
                lhs[at, bit * 8 : bit * 8 + 128] = value.astype(F32).astype(BF)

            for bit in (0, 16):
                byte_pair(rows, w, t, bit)
                if both:
                    byte_pair(pl.ds(start + 1024, 128), t, w, bit)
            return carry

        lax.fori_loop(at_row, at_row + count, body, 0)

    bit_of = lax.shift_left(1, lax.broadcasted_iota(jnp.int32, (1, 256), 1) % 8)

    def bits(rows, pair):
        cols = pl.ds(pl.multiple_of(pair * 256, 256), 256)
        byte = jnp.dot(lhs[rows], e[:, cols], preferred_element_type=F32)
        return (byte.astype(jnp.int32) & bit_of) != 0

    def mask_pair(j):
        came(gu.at[pl.ds(2 * j, 2), mine], w_loc.at[j])
        for q in (0, 1):
            keep = bits(slice(q * 1024, (q + 1) * 1024), j)
            cols = slice(q * 128, (q + 1) * 128)
            for i in (0, 1):
                v = gu[2 * j + i, mine, cols].astype(F32)
                v = jnp.where(keep[:, i * 128 : (i + 1) * 128], v, 0.0)
                gu[2 * j + i, mine, cols] = v.astype(BF)

    def swap_pair(j):
        w_remote(2 * j).start()
        w_remote(2 * j + 1).start()

    def mask_and_swap(j, carry):
        mask_pair(j)
        swap_pair(j)
        return carry

    def down_mask(k):
        if k == 0:
            d_words.wait()
            spread_words(0, 14, False)
            dn_local.wait()
        rows = slice(k * 896, (k + 1) * 896)

        def body(j, carry):
            cols = pl.ds(pl.multiple_of(j * 256, 256), 256)
            v = dn[c, rows, cols].astype(F32)
            dn[c, rows, cols] = jnp.where(bits(rows, j), v, 0.0).astype(BF)
            return carry

        lax.fori_loop(0, 4, body, 0)
        dn_remote(k).start()

    def rs_copy(s, d, u):
        return remote(
            rs.at[s, d, u], rs.at[s + 1, d, u], rs_send.at[0], rs_recv.at[s, u],
            at(xs(1 if d == 0 else -1), c, z, y),
        )

    def ag_copy(d, u, hop, block):
        return remote(
            hid.at[d, u, block], hid.at[d, u, block],
            ag_send.at[0], ag_recv.at[u, hop],
            at(xs(1 if d == 0 else -1), c, z, y),
        )

    def ag_direct(d, k, block):
        part = hid.at[d, LAST, block]
        dev = at(xs(k if d == 0 else -k), c, z, y)
        return remote(part, part, ag_send.at[0], ag_recv.at[LAST, k - 1], dev)

    def product(q, s):
        rows = slice(q * 128, (q + 1) * 128)
        blocks = (xs(-s), xs(s))
        if s == 1:
            came(tok.at[0, 0:192], af_recv.at[q, 1])
        if s == 2:
            came(tok.at[0, 0:96], af_recv.at[q, 0])

        def tile(n, carry):
            if q == 0 and s == 0:
                came(gu.at[0:2, mine], w_recv.at[n])
            for d in (0, 1):
                p[s, d, n] = jnp.dot(
                    tok[blocks[d], rows], gu[d * NT + n], preferred_element_type=F32
                )
            return carry

        lax.fori_loop(0, NT, tile, 0)

    def ring(u, s):
        part = slice((u % 4) * 32, (u % 4) * 32 + 32)
        if s:
            came(rs.at[s, :, u], rs_recv.at[s - 1, u])
        for d in (0, 1):
            if s == 0:
                rs[0, d, u] = p[0, d, :, part].astype(BF)
            elif s < 3:
                rs[s, d, u] = (rs[s, d, u].astype(F32) + p[s, d, :, part]).astype(BF)
            if s < 3:
                rs_copy(s, d, u).start()
                continue
            block = xs(1) if d == 0 else xs(-1)
            for n in range(NT):
                v = rs[3, d, u, n].astype(F32) + p[3, d, n, part]
                gate, up = v[:, :128], v[:, 128:]
                hidden = (gate / (1.0 + jnp.exp(-gate)) * up).astype(BF)
                hid[d, u, block, :, :, n * 128 : (n + 1) * 128] = hidden.reshape(2, 16, 128)
            if u == LAST:
                for k in (2, 1, 3):
                    ag_direct(d, k, block).start()
            else:
                ag_copy(d, u, 0, block).start()

    def arrived(u, hop):
        came(hid.at[:, u, 0], ag_recv.at[u, hop])
        for d in (0, 1):
            block = xs(-hop) if d == 0 else xs(hop)
            if hop < 2:
                ag_copy(d, u, hop + 1, block).start()

    def squares(q):
        def body(t, carry):
            rows = pl.ds(pl.multiple_of(q * 128 + (t % 4) * 32, 32), 32)
            v = tok[t // 4, rows].astype(F32)
            v = (v * v).reshape(4, 8, FC).sum(axis=0)
            isq[0] += v[:, :1024]
            isq[1] += v[:, 1024:]
            return carry

        lax.fori_loop(0, 16, body, 0)

    def hidden_squares(u):
        def body(t, carry):
            for d in (0, 1):
                v = hid[d, u, t].reshape(32, UH).astype(F32)
                hsq[d] += (v * v).reshape(4, 8, UH).sum(axis=0)
            return carry

        lax.fori_loop(0, NX, body, 0)

    def d_copy(u, i):
        k, h, other = i // 4, (i // 2) % 2, i % 2
        core = lax.rem(c + other, 2)
        block = lax.rem(z + k, 4)
        return remote(
            psend.at[u, core, block, h], drecv.at[u, mp], d_send.at[0], d_recv.at[u],
            at(x, core, block, 2 * c + h),
        )

    def kept_here(i):
        return jnp.logical_and(i // 4 == 0, jnp.logical_and(i % 2 == 0, y == 2 * c + (i // 2) % 2))

    first_down = next(task for task in SCHEDULE if task[0] == "down")

    def down(u, count):
        for v in range(u, u + count):
            for hop in (0, 1) if v == LAST else ():
                came(hid.at[:, v, 0], ag_recv.at[v, hop])
            arrived(v, 2)
        if ("down", u, count) == first_down:
            came(dn.at[0], dn_recv.at[0])

        for other, core in ((1, 1 - c), (0, c)):

            def tile(t, inner, core=core):
                cols = pl.ds(pl.multiple_of(t * 512, 512), 512)
                acc = sum(
                    jnp.dot(
                        hid[d, u : u + count].reshape(count * 128, UH),
                        dn[core, d * UH : (d + 1) * UH, cols],
                        preferred_element_type=F32,
                    )
                    for d in (0, 1)
                )
                acc = acc.astype(BF)
                for i in range(count):
                    part = acc[i * 128 : (i + 1) * 128].reshape(NX, 2, 16, 512)
                    psend[u + i, core, :, :, :, cols] = part
                return inner

            lax.fori_loop(0, 2, tile, 0)

            def send(i, inner, other=other):
                i = lax.rem(i + 2, 8) * 2 + other
                for v in range(u, u + count):

                    @pl.when(jnp.logical_not(kept_here(i)))
                    def _():
                        d_copy(v, i).start()

                return inner

            lax.fori_loop(0, 8, send, 0)

        @pl.when(y // 2 == c)
        def _():
            for v in range(u, u + count):
                drecv[v, mp] = psend[v, c, z, y % 2]

        for v in range(u, u + count):
            hidden_squares(v)

    def finish(u):
        here = y // 2 == c

        @pl.when(here)
        def _():
            came(drecv.at[u, 0:15], d_recv.at[u])

        @pl.when(jnp.logical_not(here))
        def _():
            came(drecv.at[u], d_recv.at[u])

        for t in range(2):
            cols = slice(t * 512, (t + 1) * 512)
            total = drecv[u, 0, :, cols].astype(F32)
            for src in range(1, 16):
                total += drecv[u, src, :, cols].astype(F32)
            out[u * 16 : (u + 1) * 16, cols] = total.astype(BF)

    def token_norms():
        copy = remote(isq.at[1 - c], isq_r, n_send.at[0], n_recv.at[0], peer)
        copy.start()
        copy.wait_recv()
        inorm[...] = jnp.sqrt(jnp.sum(isq[c] + isq_r[...], axis=0, keepdims=True))

    def hidden_norms():
        copy = remote(hsq, hsq_r, n_send.at[1], n_recv.at[1], peer)
        copy.start()
        copy.wait_recv()
        for d in (0, 1):
            hnorm[:, d * UH : (d + 1) * UH] = jnp.sqrt(
                jnp.sum(hsq[d] + hsq_r[d], axis=0, keepdims=True)
            )

    tasks = dict(
        product=product, ring=ring, hop=lambda u, h: arrived(u, h - 1), down=down,
        finish=finish, squares=squares, token_norms=token_norms, hidden_norms=hidden_norms,
        down_mask=down_mask,
    )
    tasks["pass"] = pass_on

    with jax.named_scope("words"):
        g_words.wait()
        u_words.wait()
        spread_words(0, 8, True)
        d_words.start()
    with jax.named_scope("mask0"):
        mask_pair(0)
    with jax.named_scope("barrier"):
        pl.semaphore_wait(barrier, 34)
    swap_pair(0)
    with jax.named_scope("norm"):
        gain_copy.wait()
        norm(0)
        send_tokens(0, 1)
    with jax.named_scope("mask"):
        mask_and_swap(1, 0)
    with jax.named_scope("norm"):
        norm(1)
        send_tokens(1, 1)
        send_tokens(0, 0)
        send_tokens(1, 0)
    with jax.named_scope("mask"):
        lax.fori_loop(2, NT, mask_and_swap, 0)
    with jax.named_scope("norm"):
        for g in (2, 3):
            norm(g)
            send_tokens(g, 1)
            send_tokens(g, 0)
    for task in SCHEDULE:
        with jax.named_scope("_".join(str(v) for v in task)):
            tasks[task[0]](*task[1:])

    with jax.named_scope("sent"):

        came(gu.at[:, mine], w_send.at[0])
        came(dn.at[0], dn_send.at[0])
        came(nsend, ax_send.at[0])
        came(tok.at[0:3, 0:192], af_send.at[0])
        came(rs.at[0:3], rs_send.at[0])
        came(hid.at[:, :, 0:3], ag_send.at[0])
        came(isq.at[0], n_send.at[0])
        came(hsq, n_send.at[1])

        @pl.when(y // 2 == c)
        def _():
            came(drecv.at[:, 0:15], d_send.at[0])

        @pl.when(y // 2 != c)
        def _():
            came(drecv, d_send.at[0])


def main_call(*args):
    dma = pltpu.SemaphoreType.DMA
    vm = pltpu.VMEM
    anywhere = pl.BlockSpec(memory_space=pl.ANY)
    in_vmem = pl.BlockSpec(memory_space=pltpu.VMEM)
    return pl.pallas_call(
        main_kernel,
        in_specs=[anywhere] * 8,
        out_specs=[in_vmem] * 3,
        out_shape=[
            jax.ShapeDtypeStruct((128, 1024), BF),
            jax.ShapeDtypeStruct((1, 1024), F32),
            jax.ShapeDtypeStruct((1, 1792), F32),
        ],
        scratch_shapes=[
            vm((2 * NT, FC, 256), BF),
            vm((2, 1792, 1024), BF),
            vm((NX, RT, FC), BF),
            vm((4, 2, U, NT, 32, 256), BF),
            vm((2, U, NX, 2, 16, UH), BF),
            vm((4, 2, NT, 128, 256), F32),
            vm((U, 2, NX, 2, 16, 1024), BF),
            vm((U, 16, 16, 1024), BF),
            vm((G, 2, 32, 8192), BF),
            vm((G, 2, 32, 128), F32),
            vm((G, 3, 16, FC), BF),
            vm((128, 1792), jnp.int32),
            vm((2048, 256), BF),
            vm((256, 1792), BF),
            vm((2, 8, 1024), F32),
            vm((8, 1024), F32),
            vm((2, 8, UH), F32),
            vm((2, 8, UH), F32),
            vm((1, 8192), F32),
            dma((G,)), dma((4,)), dma((NT,)), dma((1,)), dma((NT,)),
            dma((1,)), dma((1,)), dma((1,)),
            dma((1,)), dma((G, 2)), dma((1,)), dma((2, 2)),
            dma((1,)), dma((3, U)),
            dma((1,)), dma((U, 3)),
            dma((1,)), dma((U,)),
            dma((2,)), dma((2,)),
        ],
        compiler_params=pltpu.CompilerParams(
            collective_id=0, has_side_effects=True, vmem_limit_bytes=67043328
        ),
    )(*args)


def hand_out(mixed, inorm, hnorm, mixed_out, inorm_out, hnorm_out):
    mixed_out[...] = mixed[...]
    inorm_out[...] = inorm[...].reshape(1024)
    hnorm_out[...] = hnorm[...].reshape(1792)


def on_device(
    tokens, norm_gain, gate_weight, gate_mask, up_weight, up_mask, down_weight, down_mask
):
    mixed, inorm, hnorm = main_call(
        tokens, norm_gain.reshape(1, 8192), gate_weight, gate_mask.T, up_weight, up_mask.T,
        down_weight, down_mask.T,
    )
    return pl.pallas_call(
        hand_out,
        out_shape=[
            jax.ShapeDtypeStruct((128, 1024), BF),
            jax.ShapeDtypeStruct((1024,), F32),
            jax.ShapeDtypeStruct((1792,), F32),
        ],
    )(mixed, inorm, hnorm)


def solution(mesh):
    return jax.shard_map(
        on_device,
        mesh=mesh,
        in_specs=(
            P("dp", None), P(), P("dp", "mp"), P("dp", "mp"),
            P("dp", "mp"), P("dp", "mp"), P("mp", "dp"), P("mp", "dp"),
        ),
        out_specs=(P("mp", "dp"), P("dp"), P("mp")),
        check_vma=False,
    )
```
